32 devices in a mesh: gx: 8 (over z, x), gy: 2 (over core), gz: 2 (over y).
Axes of the slice: x: 2, y: 2, z: 4, core: 2. Of those that a mesh axis runs over, the one named last changes fastest.
Arguments:
- positions: float32 [16, 8, 8, 8, 3], P('gx', 'gy', 'gz'), may hold values from 0 to 1
- species: int32 [16, 8, 8, 8], P('gx', 'gy', 'gz'), may hold values from 0 to 3
- neighbors: int32 [16, 8, 8, 8, 16], P('gx', 'gy', 'gz'), may hold values from 0 to 215, as said below
- edge_mask: int32 [16, 8, 8, 8, 16], P('gx', 'gy', 'gz'), may hold values 0 or 1
- species_embed: float32 [4, 128], replicated, may hold values from -6 to 6
- radial_weight: float32 [2, 8, 384], replicated, may hold values from -6 to 6
- mix_weight: float32 [2, 384, 128], replicated, may hold values from -0.3125 to 0.3125
- readout: float32 [128], replicated, may hold values from -0.5 to 0.5
- energy_offset: float32 [4], replicated, may hold values from -6 to 6
Outputs:
- atom_energy: float32 [16, 8, 8, 8], P('gx', 'gy', 'gz')
- forces: float32 [16, 8, 8, 8, 3], P('gx', 'gy', 'gz')
The draws below stay inside these ranges and needn't reach their ends.
Inputs may be any that keep to these rules, and one draw needn't show every extreme that they name: `neighbors`: each entry lies in 0 to 215 and names slot n mod 8 of the cell at offset (n // 72 - 1, (n // 24) mod 3 - 1, (n // 8) mod 3 - 1), periodic; it never names the receiving atom itself (104 plus its own slot). Repeats may occur.
All inputs are finite; a program needn't handle non-finite values.
Results may differ from the reference program's by a relative error of at most 0.0003.
Values sent between devices are 32-bit elements.
A program may use at most 128 MiB of HBM per device.

```python
import math
import jax
import jax.numpy as jnp
from jax import lax

K = 8
E = 16
C = 128
NB = 8
S = 4
LAYERS = 2
NX = 16
NY = 8
NZ = 8


def draw_neighbors(key, part):
    arr_shape = (NX, NY, NZ, K, E)
    raw_ids = jax.random.randint(key, arr_shape, 0, 27 * K - 1, dtype=jnp.int32)
    own_slot = 13 * K + lax.broadcasted_iota(jnp.int32, arr_shape, 3)
    return raw_ids + (raw_ids >= own_slot).astype(jnp.int32)


def with_ends(values, rng, smallest, largest):
    shape = values.shape
    spot = [jax.random.randint(jax.random.fold_in(rng, axis), (), 0, shape[axis]) for axis in range(len(shape))]
    values = values.at[tuple(spot)].set(smallest)
    longest = shape.index(max(shape))
    spot[longest] = (spot[longest] + 1) % shape[longest]
    return values.at[tuple(spot)].set(largest)


def block_scale(own_key, extent, pieces, low, top_value):
    factor_of = 1.0
    for dim, parts in pieces:
        draws = jax.random.uniform(jax.random.fold_in(jax.random.fold_in(own_key, 6), dim), (parts,), jnp.float32, low / len(pieces), top_value / len(pieces))
        factor_of = factor_of * jnp.repeat(jnp.exp(draws), extent[dim] // parts).reshape((-1,) + (1,) * (len(extent) - 1 - dim))
    return factor_of


def scatter_about(rng, shape, spread, most, kind=jnp.bfloat16):
    values = jax.random.normal(rng, shape, jnp.float32) * spread
    return jnp.minimum(jnp.maximum(values, -most), most).astype(kind)


def setup_inputs(seed: int = 0) -> dict:
    arg_keys = jax.random.split(jax.random.key(seed), 10)
    return {
        "positions": jnp.clip(1.0 * jax.random.uniform(arg_keys[0], (NX, NY, NZ, K, 3), jnp.float32) ** block_scale(arg_keys[0], (NX, NY, NZ, K, 3), ((0, 8), (1, 2), (2, 2)), -0.2, 0.2), 0.0, 1.0),
        "species": with_ends(jax.random.randint(arg_keys[1], (NX, NY, NZ, K), 0, S), jax.random.fold_in(arg_keys[1], 1), 0, S - 1).astype(jnp.int32),
        "neighbors": draw_neighbors(jax.random.fold_in(arg_keys[9], 71), 0),
        "edge_mask": with_ends((jax.random.randint(arg_keys[3], (NX, NY, NZ, K, E), 0, 4) < 3).astype(jnp.int32), jax.random.fold_in(arg_keys[3], 1), 0, 1),
        "species_embed": scatter_about(arg_keys[4], (S, C), 1.0, 6.0, jnp.float32),
        "radial_weight": scatter_about(arg_keys[5], (LAYERS, NB, 3 * C), 1.0, 6.0, jnp.float32),
        "mix_weight": scatter_about(arg_keys[6], (LAYERS, 3 * C, C), (3 * C) ** -0.5, 0.3125, jnp.float32),
        "readout": scatter_about(arg_keys[7], (C,), C ** -0.5, 0.5, jnp.float32),
        "energy_offset": scatter_about(arg_keys[8], (S,), 1.0, 6.0, jnp.float32),
    }


cutoff_radius = 2.0
highest = lax.Precision.HIGHEST

def stencil_parts(neighbor_ids, slot_count):
    stencil = neighbor_ids // slot_count
    return (stencil // 9 - 1, stencil // 3 % 3 - 1, stencil % 3 - 1, neighbor_ids % slot_count)

def sender_rows(neighbor_ids, grid_y, grid_z, margin):
    arr_shape = neighbor_ids.shape
    slot_count = arr_shape[3]
    step_x, step_y, step_z, slot_id = stencil_parts(neighbor_ids, slot_count)
    cell_x = lax.broadcasted_iota(jnp.int32, arr_shape, 0) + margin + step_x
    cell_y = lax.broadcasted_iota(jnp.int32, arr_shape, 1) + margin + step_y
    cell_z = lax.broadcasted_iota(jnp.int32, arr_shape, 2) + margin + step_z
    return ((cell_x * grid_y + cell_y) * grid_z + cell_z) * slot_count + slot_id

def displacement(pos_padded, pos_own, neighbor_ids, sender_idx):
    step_x, step_y, step_z, slot_id = stencil_parts(neighbor_ids, neighbor_ids.shape[3])
    offsets = jnp.stack([step_x, step_y, step_z], -1).astype(jnp.float32)
    remote = pos_padded.reshape(-1, 3)[sender_idx]
    return offsets + remote - pos_own[..., None, :]

def edge_basis(displace, basis_count):
    radius_sq = lax.optimization_barrier(jnp.sum(displace * displace, -1))
    radius = jnp.sqrt(radius_sq)
    envelope = jnp.where(radius < cutoff_radius, (1.0 - radius_sq / cutoff_radius ** 2) ** 2, 0.0)
    centres = jnp.arange(basis_count, dtype=jnp.float32) * (cutoff_radius / (basis_count - 1))
    sharpness = ((basis_count - 1) / cutoff_radius) ** 2
    radial_basis = jnp.exp(-sharpness * (radius[..., None] - centres) ** 2) * envelope[..., None]
    scaled = displace / cutoff_radius
    along_x = scaled[..., 0]
    along_y = scaled[..., 1]
    along_z = scaled[..., 2]
    first_order = math.sqrt(3.0) * scaled
    root_15 = math.sqrt(15.0)
    second_order = jnp.stack([root_15 * along_x * along_y, root_15 * along_y * along_z, 0.5 * math.sqrt(5.0) * (3.0 * along_z * along_z - lax.optimization_barrier(jnp.sum(scaled * scaled, -1))), root_15 * along_x * along_z, 0.5 * root_15 * (along_x * along_x - along_y * along_y)], -1)
    return (radial_basis, first_order, second_order)

def interact(senders, radial_basis, first_order, second_order, edge_mask, radial_w, mix_w):
    channels = senders.shape[-1]
    radial = jnp.einsum('...k,kc->...c', radial_basis, radial_w, precision=highest)
    gate_mask = edge_mask.astype(jnp.float32)[..., None]
    term_zero = gate_mask * radial[..., :channels] * senders
    term_one = gate_mask * radial[..., channels:2 * channels] * senders
    term_two = gate_mask * radial[..., 2 * channels:] * senders
    norm_scale = senders.shape[-2] ** (-0.5)
    scalar_part = norm_scale * lax.optimization_barrier(jnp.sum(term_zero, -2))
    vector_part = norm_scale * jnp.einsum('...em,...ec->...mc', first_order, term_one, precision=highest)
    tensor_part = norm_scale * jnp.einsum('...em,...ec->...mc', second_order, term_two, precision=highest)
    invariants = jnp.concatenate([scalar_part, lax.optimization_barrier(jnp.sum(vector_part * vector_part, -2)), lax.optimization_barrier(jnp.sum(tensor_part * tensor_part, -2))], -1)
    return jax.nn.silu(jnp.einsum('...j,jc->...c', invariants, mix_w, precision=highest))

def pad_cells(values):
    margins = ((1, 1), (1, 1), (1, 1)) + ((0, 0),) * (values.ndim - 3)
    return jnp.pad(values, margins, mode='wrap')

def reference(positions, species, neighbors, edge_mask, species_embed, radial_weight, mix_weight, readout, energy_offset):
    grid_x = neighbors.shape[0]
    grid_y = neighbors.shape[1]
    grid_z = neighbors.shape[2]
    channels = species_embed.shape[1]
    sender_idx = sender_rows(neighbors, grid_y + 2, grid_z + 2, 1)
    start_feat = species_embed[species]

    def energy_of(pos_all):
        displace = displacement(pad_cells(pos_all), pos_all, neighbors, sender_idx)
        hidden = start_feat
        for layer_idx in range(LAYERS):
            feat_table = pad_cells(hidden).reshape(-1, channels)

            def slab_update(slab_idx):
                radial_basis, first_order, second_order = edge_basis(displace[slab_idx], NB)
                return interact(feat_table[sender_idx[slab_idx]], radial_basis, first_order, second_order, edge_mask[slab_idx], radial_weight[layer_idx], mix_weight[layer_idx])
            hidden = hidden + lax.map(jax.checkpoint(slab_update), jnp.arange(grid_x, dtype=jnp.int32))
        return energy_offset[species] + jnp.einsum('...c,c->...', hidden, readout, precision=highest)
    energy, pull_back = jax.vjp(energy_of, positions)
    grad_pos, = pull_back(jnp.ones_like(energy))
    return (energy, -grad_pos)
```

```python
import functools
import itertools
import math

import jax
import jax.numpy as jnp
from jax import lax
from jax.experimental import pallas as pl
from jax.experimental.pallas import tpu as pltpu
from jax.sharding import PartitionSpec as P

F32 = jnp.float32
BF16 = jnp.bfloat16
MESH = pl.DeviceIdType.MESH
AXES = ("gx", "gy", "gz")
RC = 2.0
NO_EDGE = 1023
OFFSETS = [o for o in itertools.product((-1, 0, 1), repeat=3) if any(o)]
ORDERS = ((0, 1), (1, 4), (4, 9))
VM = pl.BlockSpec(memory_space=pltpu.VMEM)

NN = ((1,), (0,))
NT = ((1,), (1,))
TN = ((0,), (0,))


def split(x):
    hi = x.astype(BF16)
    return hi, (x - hi.astype(F32)).astype(BF16)


def split32(x):
    hi = x.astype(BF16).astype(F32)
    return hi, x - hi


def mm(a, b, dims):
    return lax.dot_general(a, b, (dims, ((), ())), preferred_element_type=F32)


def mm3(a, b, dims):
    return mm(a[0], b[0], dims) + (mm(a[0], b[1], dims) + mm(a[1], b[0], dims))


def peer(o):
    ids = []
    for axis, step in zip(AXES, o):
        n = lax.axis_size(axis)
        ids.append(lax.rem(lax.axis_index(axis) + (step + n), n))
    return tuple(ids)


def greet():
    barrier = pltpu.get_barrier_semaphore()
    for o in OFFSETS:
        pl.semaphore_signal(barrier, inc=1, device_id=peer(o), device_id_type=MESH)
    pl.semaphore_wait(barrier, len(OFFSETS))


def box(o, dims, minus, zero, plus):
    out = []
    for s, n in zip(o, dims):
        out.append(zero(n) if s == 0 else (plus(n) if s > 0 else minus(n)))
    return tuple(out)


def face(o, dims):
    return box(o, dims, lambda n: pl.ds(0, 1), lambda n: pl.ds(0, n), lambda n: pl.ds(n - 1, 1))


def halo(o, dims):
    return box(o, dims, lambda n: pl.ds(0, 1), lambda n: pl.ds(1, n), lambda n: pl.ds(n + 1, 1))


def opposite(o):
    return tuple(-s for s in o)


def spread_kernel(dims, own_ref, ext_ref, send_sem, recv_sem, local_sem):
    greet()
    inner = tuple(pl.ds(1, n) for n in dims)
    local = pltpu.make_async_copy(own_ref, ext_ref.at[inner], local_sem)
    local.start()
    copies = []
    for i, o in enumerate(OFFSETS):
        copies.append(
            pltpu.make_async_remote_copy(
                src_ref=own_ref.at[face(o, dims)],
                dst_ref=ext_ref.at[halo(opposite(o), dims)],
                send_sem=send_sem.at[i],
                recv_sem=recv_sem.at[i],
                device_id=peer(o),
                device_id_type=MESH,
            )
        )
        copies[-1].start()
    local.wait()
    for copy in copies:
        copy.wait()


def spread(own, cid):
    dims = own.shape[:3]
    n = len(OFFSETS)
    return pl.pallas_call(
        functools.partial(spread_kernel, dims),
        out_shape=jax.ShapeDtypeStruct(tuple(d + 2 for d in dims) + own.shape[3:], own.dtype),
        in_specs=[VM],
        out_specs=VM,
        scratch_shapes=[
            pltpu.SemaphoreType.DMA((n,)),
            pltpu.SemaphoreType.DMA((n,)),
            pltpu.SemaphoreType.DMA,
        ],
        compiler_params=pltpu.CompilerParams(collective_id=cid, has_side_effects=True),
        name=f"spread_{cid}",
    )(own)


def fold_kernel(dims, ext_ref, own_ref, recv, send_sem, recv_sem):
    greet()
    copies = []
    for i, o in enumerate(OFFSETS):
        copies.append(
            pltpu.make_async_remote_copy(
                src_ref=ext_ref.at[halo(o, dims)],
                dst_ref=recv.at[halo(o, dims)],
                send_sem=send_sem.at[i],
                recv_sem=recv_sem.at[i],
                device_id=peer(o),
                device_id_type=MESH,
            )
        )
        copies[-1].start()
    own_ref[...] = ext_ref[tuple(pl.ds(1, n) for n in dims)]
    for o, copy in zip(OFFSETS, copies):
        copy.wait()
        at = face(opposite(o), dims)
        own_ref[at] = own_ref[at] + recv[halo(o, dims)]


def fold(ext, cid):
    dims = tuple(d - 2 for d in ext.shape[:3])
    n = len(OFFSETS)
    return pl.pallas_call(
        functools.partial(fold_kernel, dims),
        out_shape=jax.ShapeDtypeStruct(dims + ext.shape[3:], ext.dtype),
        in_specs=[VM],
        out_specs=VM,
        scratch_shapes=[
            pltpu.VMEM(ext.shape, ext.dtype),
            pltpu.SemaphoreType.DMA((n,)),
            pltpu.SemaphoreType.DMA((n,)),
        ],
        compiler_params=pltpu.CompilerParams(collective_id=cid, has_side_effects=True),
        name=f"fold_{cid}",
    )(ext)


def iota(shape, dim):
    return lax.broadcasted_iota(jnp.int32, shape, dim)


def slot_mask(slots, lanes):
    per = lanes // slots
    lane, row = iota((slots, lanes), 1), iota((slots, lanes), 0)
    return jnp.where((lane >= row * per) & (lane < row * per + per), 1.0, 0.0).astype(F32)


def basis(geom, nb):
    dx, dy, dz, ms = geom[0:1], geom[1:2], geom[2:3], geom[4:5]
    r2 = dx * dx + dy * dy + dz * dz
    r = jnp.sqrt(r2)
    inside = r < RC
    w = 1.0 - r2 * (1.0 / RC**2)
    u = jnp.where(inside, w * w, 0.0)
    mu = iota((nb, geom.shape[1]), 0).astype(F32) * (RC / (nb - 1))
    g = ((nb - 1) / RC) ** 2
    off = r - mu
    gauss = jnp.exp(-g * off * off)
    rb = gauss * u
    px, py, pz = dx / RC, dy / RC, dz / RC
    c3, c5, c15 = math.sqrt(3.0), math.sqrt(5.0), math.sqrt(15.0)
    ys = [
        ms,
        ms * (c3 * px),
        ms * (c3 * py),
        ms * (c3 * pz),
        ms * (c15 * px * py),
        ms * (c15 * py * pz),
        ms * ((0.5 * c5) * (3.0 * pz * pz - (px * px + py * py + pz * pz))),
        ms * (c15 * px * pz),
        ms * ((0.5 * c15) * (px * px - py * py)),
    ]
    return rb, ys, (r, w, inside, gauss, off, g, (px, py, pz))


def geom_pull(geom, extra, d_rb, d_y):
    r, w, inside, gauss, off, g, (px, py, pz) = extra
    ms = geom[4:5]
    du = jnp.where(inside, -r * w, 0.0)
    u = jnp.where(inside, w * w, 0.0)
    d_r = jnp.sum(d_rb * gauss * (du - 2.0 * g * off * u), 0, keepdims=True)
    c3, c5, c15 = math.sqrt(3.0), math.sqrt(5.0), math.sqrt(15.0)
    gy = [ms * d_y[m : m + 1] for m in range(9)]
    vx = c3 * gy[1] + c15 * (py * gy[4] + pz * gy[7] + px * gy[8]) - c5 * px * gy[6]
    vy = c3 * gy[2] + c15 * (px * gy[4] + pz * gy[5] - py * gy[8]) - c5 * py * gy[6]
    vz = c3 * gy[3] + c15 * (py * gy[5] + px * gy[7]) + 2.0 * c5 * pz * gy[6]
    k = d_r / jnp.maximum(r, 1e-20)
    return [v / RC + k * geom[i : i + 1] for i, v in enumerate((vx, vy, vz))]


def stack3(x, order):
    hi, lo = split32(x)
    parts = {"h": hi, "l": lo}
    rows = [parts[o] for o in order]
    pad = -(3 * x.shape[0]) % 16
    if pad:
        rows.append(jnp.zeros((pad,) + x.shape[1:], F32))
    return jnp.concatenate(rows, 0).astype(BF16)


def radial_of(rb, w_stack):
    return mm(stack3(rb, "hhl"), w_stack, TN)


def orders_of(radial, h):
    c = h.shape[1]
    return [radial[:, q * c : (q + 1) * c] * h for q in range(3)]


def block_rows(ys, mask, q):
    lo, hi = ORDERS[q]
    return jnp.concatenate([ys[m] * mask for m in range(lo, hi)], 0)


def forward_cell(ys, mask, terms, a_ref, cell):
    slots = mask.shape[0]
    at = pl.ds(pl.multiple_of(cell * slots, slots), slots)
    for q, (lo, hi) in enumerate(ORDERS):
        sums = mm3(split(block_rows(ys, mask, q)), split(terms[q]), NN)
        for m in range(lo, hi):
            a_ref[m, at, :] = sums[(m - lo) * slots : (m - lo + 1) * slots]


def invariants_of(a_ref):
    a0 = a_ref[0]
    v = a_ref[1] * a_ref[1] + a_ref[2] * a_ref[2] + a_ref[3] * a_ref[3]
    t = a_ref[4] * a_ref[4]
    for m in range(5, 9):
        t = t + a_ref[m] * a_ref[m]
    return jnp.concatenate([a0, v, t], 1)


def a_grads(a_ref, d_update, mix, g_ref):
    c = d_update.shape[1]
    d_inv = mm3(split(d_update), split(mix), NT)
    for q, (lo, hi) in enumerate(ORDERS):
        part = d_inv[:, q * c : (q + 1) * c]
        for m in range(lo, hi):
            g_ref[m] = part if q == 0 else (2.0 * part) * a_ref[m]


def backward_cell(rb, ys, mask, radial, terms, h, g_ref, w_split, cell, want_dh):
    slots = mask.shape[0]
    c = h.shape[1]
    at = pl.ds(pl.multiple_of(cell * slots, slots), slots)
    d_y, pulls = [], []
    for q, (lo, hi) in enumerate(ORDERS):
        grads = jnp.concatenate([g_ref[m, at, :] for m in range(lo, hi)], 0)
        pulls.append(mm(stack3(block_rows(ys, mask, q), "hhl"), stack3(grads, "hlh"), TN))
        if q > 0:
            full = mm3(split(grads), split(terms[q]), NT)
            for m in range(hi - lo):
                d_y.append(jnp.sum(full[m * slots : (m + 1) * slots] * mask, 0, keepdims=True))
    z = jnp.concatenate([p * h for p in pulls], 1)
    d_rb = mm3(w_split, split(z), NT)
    zero = jnp.zeros_like(d_y[0])
    d_y = jnp.concatenate([zero] + d_y + [zero] * 7, 0)
    if not want_dh:
        return d_rb, d_y, None
    d_h = pulls[0] * radial[:, :c]
    for q in (1, 2):
        d_h = d_h + pulls[q] * radial[:, q * c : (q + 1) * c]
    return d_rb, d_y, d_h


def species_rows(geom, emb):
    s = emb.shape[0]
    row = iota((16, geom.shape[1]), 0).astype(F32)
    hot = jnp.where(row == geom[3:4], 1.0, 0.0).astype(BF16)
    table = jnp.concatenate([emb, jnp.zeros((16 - s, emb.shape[1]), F32)], 0)
    hi, lo = split(table)
    return mm(hot, hi, TN) + mm(hot, lo, TN)


def stencil_of(n):
    cell = n >> 3
    ox = ((cell * 57) >> 9) - 1
    row = (cell * 43) >> 7
    oy = row - 3 * (ox + 1) - 1
    oz = cell - 3 * row - 1
    return ox, oy, oz, n & 7


def ext_hot(n, rows, base, ye, ze):
    ox, oy, oz, slot = stencil_of(n)
    at = jnp.where(n < NO_EDGE, base + (ox * ye + oy) * ze + oz, -1)
    hot = jnp.where(iota((rows, n.shape[1]), 0) == at, 1.0, 0.0)
    return hot, slot


def expand_mat(slots, lanes):
    per = lanes // slots
    row, col = iota((lanes, 3 * lanes), 0), iota((lanes, 3 * lanes), 1)
    return jnp.where((col >= row * per) & (col < row * per + per), 1.0, 0.0).astype(F32)


def silu_parts(v):
    sig = 1.0 / (1.0 + jnp.exp(-v))
    return v * sig, sig * (1.0 + v * (1.0 - sig))


def first_kernel(dims, slots, edges, nb, ext_ref, own_ref, nbr_ref, emb_ref, h0_ref, w_ref, mix_ref,
                 geom_ref, hid_ref, a_ref, dsilu_ref, own_pos):
    X, Y, Z = dims
    ye, ze = Y + 2, Z + 2
    lanes = slots * edges
    rows = (X + 2) * ye * ze
    tab = ext_ref[...]
    hi = tab.astype(BF16).astype(F32)
    mid = (tab - hi).astype(BF16).astype(F32)
    low = tab - hi - mid
    parts = [p.astype(BF16) for p in (hi, mid, low)]
    own_pos[...] = lax.dot_general(
        own_ref[...], expand_mat(slots, lanes), (NN, ((), ())),
        precision=lax.Precision.HIGHEST, preferred_element_type=F32,
    )
    mask = slot_mask(slots, lanes)
    w_stack = stack3(w_ref[...], "hlh")
    s = edges ** (-0.5)

    def column(i, carry):
        cx, cy = i // Y, i % Y
        for cz in range(Z):
            cell = i * Z + cz
            n = nbr_ref[pl.ds(cell, 1), :]
            base = ((cx + 1) * ye + cy + 1) * ze + cz + 1
            hot, slot = ext_hot(n, rows, base, ye, ze)
            hot = hot.astype(BF16)
            got = mm(parts[0], hot, TN) + mm(parts[1], hot, TN) + mm(parts[2], hot, TN)
            pick = jnp.where(iota((slots, lanes), 0) == slot, 1.0, 0.0)
            vals = [
                jnp.sum(got[k * slots : (k + 1) * slots] * pick, 0, keepdims=True)
                for k in range(4)
            ]
            ox, oy, oz, _ = stencil_of(n)
            mine = own_pos[pl.ds(cell, 1), :]
            disp = [
                o.astype(F32) + vals[k] - mine[:, k * lanes : (k + 1) * lanes]
                for k, o in enumerate((ox, oy, oz))
            ]
            ms = jnp.where(n < NO_EDGE, s, 0.0)
            zero = jnp.zeros_like(ms)
            geom = jnp.concatenate(disp + [vals[3], ms, zero, zero, zero], 0)
            geom_ref[cell] = geom
            rb, ys, _ = basis(geom, nb)
            terms = orders_of(radial_of(rb, w_stack), species_rows(geom, emb_ref[...]))
            forward_cell(ys, mask, terms, a_ref, cell)
        return carry

    lax.fori_loop(0, X * Y, column, 0)
    v = mm3(split(invariants_of(a_ref)), split(mix_ref[...]), NN)
    up, slope = silu_parts(v)
    hid_ref[...] = h0_ref[...] + up
    dsilu_ref[...] = slope


def hot_rows(n, rows):
    return jnp.where(iota((rows, n.shape[1]), 0) == n, 1.0, 0.0).astype(BF16)


def second_kernel(dims, slots, edges, nb, ext_ref, geom_ref, nbr_ref, w_ref, mix_ref, read_ref,
                  energy_ref, dext_ref, drb_ref, dy_ref, a_ref, g_ref, h_ref):
    X, Y, Z = dims
    lanes = slots * edges
    c = ext_ref.shape[-1]
    mask = slot_mask(slots, lanes)
    w_stack = stack3(w_ref[...], "hlh")
    w_split = split(w_ref[...])
    near = 27 * slots
    pad = -near % 256

    def column(i, carry):
        cx, cy = i // Y, i % Y
        for cz in range(Z):
            cell = i * Z + cz
            table = jnp.concatenate(
                [
                    ext_ref[cx + a, cy + b, pl.ds(cz, 3)].reshape(3 * slots, c)
                    for a in range(3)
                    for b in range(3)
                ]
                + [jnp.zeros((pad, c), F32)],
                0,
            )
            hot = hot_rows(nbr_ref[pl.ds(cell, 1), :], near + pad)
            both = mm(hot, jnp.concatenate(split(table), 1), TN)
            h = both[:, :c] + both[:, c:]
            h_ref[pl.ds(pl.multiple_of(cell * lanes, lanes), lanes), :] = h
            rb, ys, _ = basis(geom_ref[cell], nb)
            terms = orders_of(radial_of(rb, w_stack), h)
            forward_cell(ys, mask, terms, a_ref, cell)
        return carry

    lax.fori_loop(0, X * Y, column, 0)
    v = mm3(split(invariants_of(a_ref)), split(mix_ref[...]), NN)
    up, slope = silu_parts(v)
    hid1 = ext_ref[1 : X + 1, 1 : Y + 1, 1 : Z + 1].reshape(X * Y * Z * slots, c)
    energy_ref[...] = jnp.sum((hid1 + up) * read_ref[...], 1, keepdims=True)
    a_grads(a_ref, slope * read_ref[...], mix_ref[...], g_ref)
    dext_ref[...] = jnp.zeros_like(dext_ref)

    def back(i, carry):
        cx, cy = i // Y, i % Y
        for cz in range(Z):
            cell = i * Z + cz
            h = h_ref[pl.ds(pl.multiple_of(cell * lanes, lanes), lanes), :]
            rb, ys, _ = basis(geom_ref[cell], nb)
            radial = radial_of(rb, w_stack)
            terms = orders_of(radial, h)
            d_rb, d_y, d_h = backward_cell(
                rb, ys, mask, radial, terms, h, g_ref, w_split, cell, True
            )
            drb_ref[cell] = d_rb
            dy_ref[cell] = d_y
            hot = hot_rows(nbr_ref[pl.ds(cell, 1), :], near + pad)
            both = mm(hot, jnp.concatenate(split(d_h), 1), NN)
            sums = both[:, :c] + both[:, c:]
            for j, (a, b) in enumerate(itertools.product(range(3), repeat=2)):
                at = (cx + a, cy + b, pl.ds(cz, 3))
                part = sums[j * 3 * slots : (j + 1) * 3 * slots].reshape(3, slots, c)
                dext_ref[at] = dext_ref[at] + part
        return carry

    lax.fori_loop(0, X * Y, back, 0)


def third_kernel(dims, slots, edges, nb, dh_ref, a_ref, dsilu_ref, geom_ref, nbr_ref, drb_ref, dy_ref,
                 emb_ref, w_ref, mix_ref, read_ref, sent_ref, got_ref, g_ref, eg_ref):
    X, Y, Z = dims
    ye, ze = Y + 2, Z + 2
    lanes = slots * edges
    rows = (X + 2) * ye * ze
    mask = slot_mask(slots, lanes)
    w_stack = stack3(w_ref[...], "hlh")
    w_split = split(w_ref[...])
    a_grads(a_ref, dsilu_ref[...] * (dh_ref[...] + read_ref[...]), mix_ref[...], g_ref)
    sent_ref[...] = jnp.zeros_like(sent_ref)

    def back(i, carry):
        cx, cy = i // Y, i % Y
        for cz in range(Z):
            cell = i * Z + cz
            geom = geom_ref[cell]
            rb, ys, extra = basis(geom, nb)
            h = species_rows(geom, emb_ref[...])
            radial = radial_of(rb, w_stack)
            terms = orders_of(radial, h)
            d_rb, d_y, _ = backward_cell(
                rb, ys, mask, radial, terms, h, g_ref, w_split, cell, False
            )
            grads = geom_pull(geom, extra, d_rb + drb_ref[cell], d_y + dy_ref[cell])
            eg_ref[pl.ds(cell, 1), :] = jnp.concatenate(grads, 1)
            n = nbr_ref[pl.ds(cell, 1), :]
            base = ((cx + 1) * ye + cy + 1) * ze + cz + 1
            hot, slot = ext_hot(n, rows, base, ye, ze)
            hot = hot.astype(BF16)
            pick = jnp.where(iota((slots, lanes), 0) == slot, 1.0, 0.0)
            x = jnp.concatenate([g * pick for g in grads] + [jnp.zeros((lanes - 3 * slots, lanes), F32)], 0)
            hi, lo = split(x)
            sent_ref[...] += mm(hot, hi, NT) + mm(hot, lo, NT)
        return carry

    lax.fori_loop(0, X * Y, back, 0)
    got_ref[...] = lax.dot_general(
        eg_ref[...], expand_mat(slots, lanes), (NT, ((), ())),
        precision=lax.Precision.HIGHEST, preferred_element_type=F32,
    )


def call(body, outs, scratch, name, *args):
    return pl.pallas_call(
        body,
        out_shape=[jax.ShapeDtypeStruct(s, F32) for s in outs],
        in_specs=[VM] * len(args),
        out_specs=[VM] * len(outs),
        scratch_shapes=[pltpu.VMEM(s, F32) for s in scratch],
        compiler_params=pltpu.CompilerParams(vmem_limit_bytes=56 * 1024 * 1024),
        name=name,
    )(*args)


def shards(positions, species, neighbors, edge_mask, species_embed, radial_weight, mix_weight, readout, energy_offset):
    X, Y, Z, slots, edges = neighbors.shape
    dims = (X, Y, Z)
    cells = X * Y * Z
    atoms = cells * slots
    lanes = slots * edges
    c = species_embed.shape[1]
    nb = radial_weight.shape[1]
    ext = (X + 2, Y + 2, Z + 2)
    rows = ext[0] * ext[1] * ext[2]

    nbr = jnp.where(edge_mask != 0, neighbors, NO_EDGE).reshape(cells, lanes)
    four = jnp.concatenate([positions, species[..., None].astype(F32)], -1)
    own_tab = jnp.swapaxes(four, -1, -2).reshape(cells, 4 * slots)
    own_tab = jnp.pad(own_tab, ((0, 0), (0, lanes - 4 * slots)))
    ext_tab = spread(own_tab.reshape(X, Y, Z, 1, lanes), 1).reshape(rows, lanes)
    flat_species = species.reshape(atoms, 1)
    h0 = jnp.zeros((atoms, c), F32)
    offset = jnp.zeros((atoms, 1), F32)
    for s in range(species_embed.shape[0]):
        h0 = jnp.where(flat_species == s, species_embed[s], h0)
        offset = jnp.where(flat_species == s, energy_offset[s], offset)
    size = (dims, slots, edges, nb)
    read = readout.reshape(1, c)
    geom, hid1, a0, dsilu = call(
        functools.partial(first_kernel, *size),
        [(cells, 8, lanes), (atoms, c), (9, atoms, c), (atoms, c)],
        [(cells, 3 * lanes)],
        "first",
        ext_tab, own_tab, nbr, species_embed, h0, radial_weight[0], mix_weight[0],
    )
    hid_ext = spread(hid1.reshape(X, Y, Z, slots, c), 2)
    energy, d_ext, d_rb, d_y = call(
        functools.partial(second_kernel, *size),
        [(atoms, 1), ext + (slots, c), (cells, nb, lanes), (cells, 16, lanes)],
        [(9, atoms, c), (9, atoms, c), (cells * lanes, c)],
        "second",
        hid_ext, geom, nbr, radial_weight[1], mix_weight[1], read,
    )
    d_h = fold(d_ext, 3).reshape(atoms, c)
    sent, got = call(
        functools.partial(third_kernel, *size),
        [(rows, lanes), (cells, lanes)],
        [(9, atoms, c), (cells, 3 * lanes)],
        "third",
        d_h, a0, dsilu, geom, nbr, d_rb, d_y, species_embed, radial_weight[0], mix_weight[0], read,
    )
    back = fold(sent.reshape(ext + (1, lanes)), 4).reshape(cells, lanes)
    forces = (got - back)[:, : 3 * slots].reshape(X, Y, Z, 3, slots)
    energy = energy + offset
    return energy.reshape(X, Y, Z, slots), jnp.swapaxes(forces, -1, -2)


def solution(mesh):
    g = P("gx", "gy", "gz")
    return jax.shard_map(
        shards,
        mesh=mesh,
        in_specs=(g, g, g, g, P(), P(), P(), P(), P()),
        out_specs=(g, g),
        check_vma=False,
    )
```

```python
import functools
import itertools
import math

import jax
import jax.numpy as jnp
from jax import lax
from jax.experimental import pallas as pl
from jax.experimental.pallas import tpu as pltpu
from jax.sharding import PartitionSpec as P

F32 = jnp.float32
BF16 = jnp.bfloat16
MESH = pl.DeviceIdType.MESH
AXES = ("gx", "gy", "gz")
RC = 2.0
NO_EDGE = 1023
OFFSETS = [o for o in itertools.product((-1, 0, 1), repeat=3) if any(o)]
ORDERS = ((0, 1), (1, 4), (4, 9))
VM = pl.BlockSpec(memory_space=pltpu.VMEM)

NN = ((1,), (0,))
NT = ((1,), (1,))
TN = ((0,), (0,))


def split(x):
    hi = x.astype(BF16)
    return hi, (x - hi.astype(F32)).astype(BF16)


def split32(x):
    hi = x.astype(BF16).astype(F32)
    return hi, x - hi


def mm(a, b, dims):
    return lax.dot_general(a, b, (dims, ((), ())), preferred_element_type=F32)


def mm3(a, b, dims):
    return mm(a[0], b[0], dims) + (mm(a[0], b[1], dims) + mm(a[1], b[0], dims))


def peer(o):
    ids = []
    for axis, step in zip(AXES, o):
        n = lax.axis_size(axis)
        ids.append(lax.rem(lax.axis_index(axis) + (step + n), n))
    return tuple(ids)


def greet():
    barrier = pltpu.get_barrier_semaphore()
    for o in OFFSETS:
        pl.semaphore_signal(barrier, inc=1, device_id=peer(o), device_id_type=MESH)
    pl.semaphore_wait(barrier, len(OFFSETS))


def box(o, dims, minus, zero, plus):
    out = []
    for s, n in zip(o, dims):
        out.append(zero(n) if s == 0 else (plus(n) if s > 0 else minus(n)))
    return tuple(out)


def face(o, dims):
    return box(o, dims, lambda n: pl.ds(0, 1), lambda n: pl.ds(0, n), lambda n: pl.ds(n - 1, 1))


def halo(o, dims):
    return box(o, dims, lambda n: pl.ds(0, 1), lambda n: pl.ds(1, n), lambda n: pl.ds(n + 1, 1))


def opposite(o):
    return tuple(-s for s in o)


def iota(shape, dim):
    return lax.broadcasted_iota(jnp.int32, shape, dim)


def slot_mask(slots, lanes):
    per = lanes // slots
    lane, row = iota((slots, lanes), 1), iota((slots, lanes), 0)
    return jnp.where((lane >= row * per) & (lane < row * per + per), 1.0, 0.0).astype(F32)


def basis(geom, nb):
    dx, dy, dz, ms = geom[0:1], geom[1:2], geom[2:3], geom[4:5]
    r2 = dx * dx + dy * dy + dz * dz
    r = jnp.sqrt(r2)
    inside = r < RC
    w = 1.0 - r2 * (1.0 / RC**2)
    u = jnp.where(inside, w * w, 0.0)
    mu = iota((nb, geom.shape[1]), 0).astype(F32) * (RC / (nb - 1))
    g = ((nb - 1) / RC) ** 2
    off = r - mu
    gauss = jnp.exp(-g * off * off)
    rb = gauss * u
    px, py, pz = dx / RC, dy / RC, dz / RC
    c3, c5, c15 = math.sqrt(3.0), math.sqrt(5.0), math.sqrt(15.0)
    ys = [
        ms,
        ms * (c3 * px),
        ms * (c3 * py),
        ms * (c3 * pz),
        ms * (c15 * px * py),
        ms * (c15 * py * pz),
        ms * ((0.5 * c5) * (3.0 * pz * pz - (px * px + py * py + pz * pz))),
        ms * (c15 * px * pz),
        ms * ((0.5 * c15) * (px * px - py * py)),
    ]
    return rb, ys, (r, w, inside, gauss, off, g, (px, py, pz))


def geom_pull(geom, extra, d_rb, d_y):
    r, w, inside, gauss, off, g, (px, py, pz) = extra
    ms = geom[4:5]
    du = jnp.where(inside, -r * w, 0.0)
    u = jnp.where(inside, w * w, 0.0)
    d_r = jnp.sum(d_rb * gauss * (du - 2.0 * g * off * u), 0, keepdims=True)
    c3, c5, c15 = math.sqrt(3.0), math.sqrt(5.0), math.sqrt(15.0)
    gy = [ms * d_y[m : m + 1] for m in range(9)]
    vx = c3 * gy[1] + c15 * (py * gy[4] + pz * gy[7] + px * gy[8]) - c5 * px * gy[6]
    vy = c3 * gy[2] + c15 * (px * gy[4] + pz * gy[5] - py * gy[8]) - c5 * py * gy[6]
    vz = c3 * gy[3] + c15 * (py * gy[5] + px * gy[7]) + 2.0 * c5 * pz * gy[6]
    k = d_r / jnp.maximum(r, 1e-20)
    return [v / RC + k * geom[i : i + 1] for i, v in enumerate((vx, vy, vz))]


def stack3(x, order):
    hi, lo = split32(x)
    parts = {"h": hi, "l": lo}
    rows = [parts[o] for o in order]
    pad = -(3 * x.shape[0]) % 16
    if pad:
        rows.append(jnp.zeros((pad,) + x.shape[1:], F32))
    return jnp.concatenate(rows, 0).astype(BF16)


def invariants_of(a_ref):
    a0 = a_ref[0]
    v = a_ref[1] * a_ref[1] + a_ref[2] * a_ref[2] + a_ref[3] * a_ref[3]
    t = a_ref[4] * a_ref[4]
    for m in range(5, 9):
        t = t + a_ref[m] * a_ref[m]
    return jnp.concatenate([a0, v, t], 1)


def a_grads(a_ref, d_update, mix, g_ref):
    c = d_update.shape[1]
    d_inv = mm3(split(d_update), split(mix), NT)
    for q, (lo, hi) in enumerate(ORDERS):
        part = d_inv[:, q * c : (q + 1) * c]
        for m in range(lo, hi):
            g_ref[m] = part if q == 0 else (2.0 * part) * a_ref[m]


def stencil_of(n):
    cell = n >> 3
    ox = ((cell * 57) >> 9) - 1
    row = (cell * 43) >> 7
    oy = row - 3 * (ox + 1) - 1
    oz = cell - 3 * row - 1
    return ox, oy, oz, n & 7


def ext_hot(n, rows, base, ye, ze):
    ox, oy, oz, slot = stencil_of(n)
    at = jnp.where(n < NO_EDGE, base + (ox * ye + oy) * ze + oz, -1)
    hot = jnp.where(iota((rows, n.shape[1]), 0) == at, 1.0, 0.0)
    return hot, slot


def expand_mat(slots, lanes):
    per = lanes // slots
    row, col = iota((lanes, 3 * lanes), 0), iota((lanes, 3 * lanes), 1)
    return jnp.where((col >= row * per) & (col < row * per + per), 1.0, 0.0).astype(F32)


def silu_parts(v):
    sig = 1.0 / (1.0 + jnp.exp(-v))
    return v * sig, sig * (1.0 + v * (1.0 - sig))


def hot_rows(n, rows):
    return jnp.where(iota((rows, n.shape[1]), 0) == n, 1.0, 0.0).astype(BF16)


def radial_of(rb, w_stack):
    return mm(stack3(rb, "hhl"), w_stack, TN)


def rows_hl(x):
    hi, lo = split32(x)
    return jnp.concatenate([hi, lo], 0).astype(BF16)


def order_rows(ys, mask, q):
    lo, hi = ORDERS[q]
    return jnp.concatenate([ys[m] * mask for m in range(lo, hi)], 0)


def exchange(src, dst, src_at, dst_at, send_sem, recv_sem, base):
    copies = []
    for i, o in enumerate(OFFSETS):
        copies.append(
            pltpu.make_async_remote_copy(
                src_ref=src.at[src_at(o)],
                dst_ref=dst.at[dst_at(o)],
                send_sem=send_sem.at[base + i],
                recv_sem=recv_sem.at[base + i],
                device_id=peer(o),
                device_id_type=MESH,
            )
        )
        copies[-1].start()
    return copies


def kernel(dims, slots, edges, nb, own5_ref, own_ref, nbr_ref, spec_ref, emb_ref, w_ref, mix_ref, read_ref,
           off_ref, energy_ref, force_ref,
           tab_ext, tab2, own_pos, hot_ref, hotx_ref, geom_ref, ym_ref, we_ref, v_ref, a_ref, g_ref,
           dsilu_ref, hid_own, hid_ext, rad_ref, h_ref, t_ref, z_ref, dext, drecv, drb_ref, dy_ref,
           dh_ref, eg_ref, sent, sent5, srecv, fold5, send_sem, recv_sem, local_sem):
    X, Y, Z = dims
    cells = X * Y * Z
    atoms = cells * slots
    ye, ze = Y + 2, Z + 2
    rows = (X + 2) * ye * ze
    lanes = slots * edges
    c = mix_ref.shape[-1]
    ns = emb_ref.shape[0]
    near = 27 * slots
    near_pad = hot_ref.shape[1]
    n_o = len(OFFSETS)
    s = edges ** (-0.5)
    mask = slot_mask(slots, lanes)
    own_face = lambda o: face(o, dims)
    own_in = lambda o: halo(opposite(o), dims)
    ext_face = lambda o: halo(o, dims)
    inner = tuple(pl.ds(1, n) for n in dims)
    grid = list(itertools.product(*[range(d + 2) for d in dims]))

    barrier = pltpu.get_barrier_semaphore()
    for o in OFFSETS:
        pl.semaphore_signal(barrier, inc=1, device_id=peer(o), device_id_type=MESH)

    def base_of(cx, cy, cz):
        return ((cx + 1) * ye + cy + 1) * ze + cz + 1

    def loop(body):
        def step(i, carry):
            cx, cy = i // Y, i % Y
            body(i, cx, cy)
            return carry
        lax.fori_loop(0, X * Y, step, 0)

    def edge_rows(cell):
        return pl.ds(pl.multiple_of(cell * lanes, lanes), lanes)

    def atom_rows(cell):
        return pl.ds(pl.multiple_of(cell * slots, slots), slots)

    def build_hot(i, cx, cy):
        for cz in range(Z):
            cell = i * Z + cz
            n = nbr_ref[pl.ds(cell, 1), :]
            hot_ref[cell] = hot_rows(n, near_pad)
            hotx_ref[cell] = ext_hot(n, rows, base_of(cx, cy, cz), ye, ze)[0].astype(BF16)

    loop(build_hot)
    pl.semaphore_wait(barrier, n_o)

    local = pltpu.make_async_copy(own5_ref, tab_ext.at[inner], local_sem.at[0])
    local.start()
    copies = exchange(own5_ref, tab_ext, own_face, own_in, send_sem, recv_sem, 0)
    own_pos[...] = lax.dot_general(
        own_ref[...], expand_mat(slots, lanes), (NN, ((), ())),
        precision=lax.Precision.HIGHEST, preferred_element_type=F32,
    )
    emb = emb_ref[...]
    for k in range(ns):
        wide = jnp.concatenate([emb[k : k + 1]] * 3, 1)
        we_ref[k * nb : (k + 1) * nb, :] = w_ref[0] * wide
    spec_row = spec_ref[...]
    spec_hot = jnp.where(iota((16, atoms), 0) == spec_row, 1.0, 0.0).astype(BF16)
    emb_hi, emb_lo = split(jnp.concatenate([emb, jnp.zeros((16 - ns, c), F32)], 0))
    h0 = mm(spec_hot, emb_hi, TN) + mm(spec_hot, emb_lo, TN)
    eye = jnp.where(iota((4 * slots, lanes), 0) == iota((4 * slots, lanes), 1), 1.0, 0.0).astype(BF16)
    local.wait()
    for copy in copies:
        copy.wait()

    for r, at in enumerate(grid):
        tab2[r : r + 1, :] = tab_ext[at]
    tab = tab2[...]
    hi, rest = split32(tab)
    mid, low = split32(rest)
    tab_t = jnp.concatenate([mm(eye, p.astype(BF16), NT) for p in (hi, mid, low)], 0).astype(BF16)

    def rb_species(rb, geom):
        return jnp.concatenate([jnp.where(geom[3:4] == float(k), rb, 0.0) for k in range(ns)], 0)

    def layer0(i, cx, cy):
        for cz in range(Z):
            cell = i * Z + cz
            n = nbr_ref[pl.ds(cell, 1), :]
            got = mm(tab_t, hotx_ref[cell], NN)
            got = got[: 4 * slots] + got[4 * slots : 8 * slots] + got[8 * slots :]
            ox, oy, oz, slot = stencil_of(n)
            pick = iota((slots, lanes), 0) == slot
            vals = [
                jnp.sum(jnp.where(pick, got[k * slots : (k + 1) * slots], 0.0), 0, keepdims=True)
                for k in range(4)
            ]
            mine = own_pos[pl.ds(cell, 1), :]
            disp = [
                o.astype(F32) + vals[k] - mine[:, k * lanes : (k + 1) * lanes]
                for k, o in enumerate((ox, oy, oz))
            ]
            ms = jnp.where(n < NO_EDGE, s, 0.0)
            zero = jnp.zeros_like(ms)
            geom = jnp.concatenate(disp + [vals[3], ms, zero, zero, zero], 0)
            geom_ref[cell] = geom
            rb, ys, _ = basis(geom, nb)
            blocks = [rows_hl(order_rows(ys, mask, q)) for q in range(3)]
            ym = jnp.concatenate(blocks, 0)
            ym_ref[cell] = ym
            rbs = rb_species(rb, geom)
            v = mm(ym, rows_hl(rbs), NT)
            w = ns * nb
            v = v[:, :w] + v[:, w : 2 * w]
            at = 0
            for lo, hi in ORDERS:
                span = (hi - lo) * slots
                part = v[at : at + span] + v[at + span : at + 2 * span]
                at += 2 * span
                for m in range(lo, hi):
                    v_ref[m, atom_rows(cell), :] = part[(m - lo) * slots : (m - lo + 1) * slots]

    loop(layer0)
    for q, (lo, hi) in enumerate(ORDERS):
        part = split(we_ref[:, q * c : (q + 1) * c])
        for m in range(lo, hi):
            a_ref[0, m] = mm3(split(v_ref[m]), part, NN)
    v = mm3(split(invariants_of(a_ref.at[0])), split(mix_ref[0]), NN)
    up, slope = silu_parts(v)
    dsilu_ref[...] = slope
    hid1 = h0 + up
    hid_own[...] = hid1.reshape(X, Y, Z, slots, c)
    local = pltpu.make_async_copy(hid_own, hid_ext.at[inner], local_sem.at[1])
    local.start()
    copies = exchange(hid_own, hid_ext, own_face, own_in, send_sem, recv_sem, n_o)

    w1 = w_ref[1]
    w_stack = stack3(w1, "hlh")

    def radials(i, cx, cy):
        for cz in range(Z):
            cell = i * Z + cz
            rb, _, _ = basis(geom_ref[cell], nb)
            rad_ref[edge_rows(cell), :] = radial_of(rb, w_stack)

    loop(radials)
    local.wait()
    for copy in copies:
        copy.wait()

    def layer1(i, cx, cy):
        for cz in range(Z):
            cell = i * Z + cz
            table = jnp.concatenate(
                [
                    hid_ext[cx + a, cy + b, pl.ds(cz, 3)].reshape(3 * slots, c)
                    for a in range(3)
                    for b in range(3)
                ]
                + [jnp.zeros((near_pad - near, c), F32)],
                0,
            )
            both = mm(hot_ref[cell], jnp.concatenate(split(table), 1), TN)
            h = both[:, :c] + both[:, c:]
            h_ref[edge_rows(cell), :] = h
            ym = ym_ref[cell]
            at = 0
            for q, (lo, hi) in enumerate(ORDERS):
                t = rad_ref[edge_rows(cell), q * c : (q + 1) * c] * h
                t_hi, t_lo = split(t)
                t_ref[cell, q, :lanes, :] = t_hi
                t_ref[cell, q, lanes:, :] = t_lo
                span = (hi - lo) * slots
                sums = mm(ym[at : at + 2 * span], jnp.concatenate([t_hi, t_lo], 1), NN)
                at += 2 * span
                sums = sums[:, :c] + sums[:, c:]
                sums = sums[:span] + sums[span:]
                for m in range(lo, hi):
                    a_ref[1, m, atom_rows(cell), :] = sums[(m - lo) * slots : (m - lo + 1) * slots]

    loop(layer1)
    read = read_ref[...]
    v = mm3(split(invariants_of(a_ref.at[1])), split(mix_ref[1]), NN)
    up, slope = silu_parts(v)
    a_grads(a_ref.at[1], slope * read, mix_ref[1], g_ref)
    dext[...] = jnp.zeros_like(dext)

    def back1(i, cx, cy):
        for cz in range(Z):
            cell = i * Z + cz
            h = h_ref[edge_rows(cell), :]
            ym = ym_ref[cell]
            d_h = None
            at = 0
            for q, (lo, hi) in enumerate(ORDERS):
                span = (hi - lo) * slots
                grads = jnp.concatenate([g_ref[m, atom_rows(cell), :] for m in range(lo, hi)], 0)
                g_hi, g_lo = split32(grads)
                yq = ym[at : at + 2 * span]
                at += 2 * span
                lhs = jnp.concatenate([yq, yq], 0)
                rhs = jnp.concatenate([g_hi, g_hi, g_lo, g_lo], 0).astype(BF16)
                pull = mm(lhs, rhs, TN)
                term = pull * rad_ref[edge_rows(cell), q * c : (q + 1) * c]
                d_h = term if d_h is None else d_h + term
                z_hi, z_lo = split(pull * h)
                z_ref[cell, :lanes, q * c : (q + 1) * c] = z_hi
                z_ref[cell, lanes:, q * c : (q + 1) * c] = z_lo
            both = mm(hot_ref[cell], jnp.concatenate(split(d_h), 1), NN)
            sums = both[:, :c] + both[:, c:]
            for j, (a, b) in enumerate(itertools.product(range(3), repeat=2)):
                at = (cx + a, cy + b, pl.ds(cz, 3))
                part = sums[j * 3 * slots : (j + 1) * 3 * slots].reshape(3, slots, c)
                dext[at] = dext[at] + part

    loop(back1)
    copies = exchange(dext, drecv, ext_face, ext_face, send_sem, recv_sem, 2 * n_o)

    hid2 = hid_ext[1 : X + 1, 1 : Y + 1, 1 : Z + 1].reshape(atoms, c) + up
    read8 = jnp.concatenate([read] * 8, 0)
    energy = mm3(split(read8), split(hid2), NT)[0:1]
    for k in range(ns):
        energy = energy + jnp.where(spec_row == k, off_ref[0, k], 0.0)
    energy_ref[...] = energy
    w_rows = rows_hl(w1)

    def pull_rows(full, first, count):
        return [
            jnp.sum(full[m * slots : (m + 1) * slots] * mask, 0, keepdims=True)
            for m in range(first, first + count)
        ]

    def geom1(i, cx, cy):
        for cz in range(Z):
            cell = i * Z + cz
            d = mm(w_rows, z_ref[cell], NT)
            d = d[:, :lanes] + d[:, lanes:]
            drb_ref[cell] = d[:nb] + d[nb:]
            d_y = [jnp.zeros((1, lanes), F32)]
            for q in (1, 2):
                lo, hi = ORDERS[q]
                grads = jnp.concatenate([g_ref[m, atom_rows(cell), :] for m in range(lo, hi)], 0)
                full = mm(rows_hl(grads), t_ref[cell, q], NT)
                full = full[:, :lanes] + full[:, lanes:]
                span = (hi - lo) * slots
                d_y += pull_rows(full[:span] + full[span:], 0, hi - lo)
            dy_ref[cell] = jnp.concatenate(d_y + [d_y[0]] * 7, 0)

    loop(geom1)
    dh_ref[...] = dext[inner]
    for o, copy in zip(OFFSETS, copies):
        copy.wait()
        at = face(opposite(o), dims)
        dh_ref[at] = dh_ref[at] + drecv[halo(o, dims)]

    cot = dh_ref[...].reshape(atoms, c) + read
    a_grads(a_ref.at[0], dsilu_ref[...] * cot, mix_ref[0], g_ref)
    for q, (lo, hi) in enumerate(ORDERS):
        part = split(we_ref[:, q * c : (q + 1) * c])
        for m in range(lo, hi):
            v_ref[m] = mm3(split(g_ref[m]), part, NT)
    sent[...] = jnp.zeros_like(sent)

    def back0(i, cx, cy):
        hots, xs = [], []
        for cz in range(Z):
            cell = i * Z + cz
            geom = geom_ref[cell]
            rb, ys, extra = basis(geom, nb)
            rbs = rb_species(rb, geom)
            d_v = jnp.concatenate([v_ref[m, atom_rows(cell), :] for m in range(9)], 0)
            d_v = split32(d_v)
            r_v = split32(rbs)
            lhs = jnp.concatenate([d_v[0], d_v[1]], 0).astype(BF16)
            rhs = jnp.concatenate([r_v[0], r_v[1]], 1).astype(BF16)
            full = mm(lhs, rhs, NN)
            full = full[:, :lanes] + full[:, lanes:]
            full = full[: 9 * slots] + full[9 * slots :]
            d_y = [jnp.zeros((1, lanes), F32)] + pull_rows(full, 1, 8)
            yall = jnp.concatenate([y * mask for y in ys], 0)
            d_rbs = mm(
                jnp.concatenate([d_v[0], d_v[0], d_v[1], jnp.zeros((slots, ns * nb), F32)], 0).astype(BF16),
                stack3(yall, "hlh"),
                TN,
            )
            d_rb = drb_ref[cell]
            for k in range(ns):
                d_rb = d_rb + jnp.where(geom[3:4] == float(k), d_rbs[k * nb : (k + 1) * nb], 0.0)
            d_y = jnp.concatenate(d_y + [d_y[0]] * 7, 0) + dy_ref[cell]
            grads = geom_pull(geom, extra, d_rb, d_y)
            eg_ref[pl.ds(cell, 1), :] = jnp.concatenate(grads, 1)
            slot = stencil_of(nbr_ref[pl.ds(cell, 1), :])[3]
            pick = iota((slots, lanes), 0) == slot
            zero = jnp.zeros((slots, lanes), F32)
            x_hi, x_lo = split32(jnp.concatenate([jnp.where(pick, g, 0.0) for g in grads] + [zero], 0))
            hot = hotx_ref[cell]
            hots += [hot, hot]
            xs += [x_hi.astype(BF16), x_lo.astype(BF16)]
        sent[...] += mm(jnp.concatenate(hots, 1), jnp.concatenate(xs, 1), NT)

    loop(back0)
    sent5[...] = jnp.zeros_like(sent5)
    width = sent.shape[1]
    for r, at in enumerate(grid):
        sent5[at + (slice(None), slice(0, width))] = sent[r : r + 1, :]
    copies = exchange(sent5, srecv, ext_face, ext_face, send_sem, recv_sem, 3 * n_o)
    force_ref[...] = lax.dot_general(
        eg_ref[...], expand_mat(slots, lanes), (NT, ((), ())),
        precision=lax.Precision.HIGHEST, preferred_element_type=F32,
    )
    fold5[...] = sent5[inner]
    for o, copy in zip(OFFSETS, copies):
        copy.wait()
        at = face(opposite(o), dims)
        fold5[at] = fold5[at] + srecv[halo(o, dims)]
    for r, at in enumerate(itertools.product(*[range(d) for d in dims])):
        force_ref[r : r + 1, :] = force_ref[r : r + 1, :] - fold5[at]


def shards(positions, species, neighbors, edge_mask, species_embed, radial_weight, mix_weight, readout, energy_offset):
    X, Y, Z, slots, edges = neighbors.shape
    dims = (X, Y, Z)
    cells = X * Y * Z
    atoms = cells * slots
    lanes = slots * edges
    ns, c = species_embed.shape
    nb = radial_weight.shape[1]
    ext = (X + 2, Y + 2, Z + 2)
    rows = ext[0] * ext[1] * ext[2]
    near = -(-27 * slots // 256) * 256

    nbr = jnp.where(edge_mask != 0, neighbors, NO_EDGE).reshape(cells, lanes)
    four = jnp.concatenate([positions, species[..., None].astype(F32)], -1)
    own_tab = jnp.swapaxes(four, -1, -2).reshape(cells, 4 * slots)
    own_tab = jnp.pad(own_tab, ((0, 0), (0, lanes - 4 * slots)))
    vm = pltpu.VMEM
    count = 4 * len(OFFSETS)
    smem = pl.BlockSpec(memory_space=pltpu.SMEM)
    energy, forces = pl.pallas_call(
        functools.partial(kernel, dims, slots, edges, nb),
        out_shape=[jax.ShapeDtypeStruct((1, atoms), F32), jax.ShapeDtypeStruct((cells, lanes), F32)],
        in_specs=[VM] * 8 + [smem],
        out_specs=[VM, VM],
        scratch_shapes=[
            vm(ext + (1, lanes), F32),
            vm((rows, lanes), F32),
            vm((cells, 3 * lanes), F32),
            vm((cells, near, lanes), BF16),
            vm((cells, rows, lanes), BF16),
            vm((cells, 8, lanes), F32),
            vm((cells, 18 * slots, lanes), BF16),
            vm((ns * nb, 3 * c), F32),
            vm((9, atoms, ns * nb), F32),
            vm((2, 9, atoms, c), F32),
            vm((9, atoms, c), F32),
            vm((atoms, c), F32),
            vm(dims + (slots, c), F32),
            vm(ext + (slots, c), F32),
            vm((cells * lanes, 3 * c), F32),
            vm((cells * lanes, c), F32),
            vm((cells, 3, 2 * lanes, c), BF16),
            vm((cells, 2 * lanes, 3 * c), BF16),
            vm(ext + (slots, c), F32),
            vm(ext + (slots, c), F32),
            vm((cells, nb, lanes), F32),
            vm((cells, 16, lanes), F32),
            vm(dims + (slots, c), F32),
            vm((cells, 3 * lanes), F32),
            vm((rows, 4 * slots), F32),
            vm(ext + (1, lanes), F32),
            vm(ext + (1, lanes), F32),
            vm(dims + (1, lanes), F32),
            pltpu.SemaphoreType.DMA((count,)),
            pltpu.SemaphoreType.DMA((count,)),
            pltpu.SemaphoreType.DMA((2,)),
        ],
        compiler_params=pltpu.CompilerParams(
            collective_id=1, has_side_effects=True, vmem_limit_bytes=58 * 1024 * 1024
        ),
        name="potential",
    )(
        own_tab.reshape(X, Y, Z, 1, lanes), own_tab, nbr, species.reshape(1, atoms), species_embed,
        radial_weight, mix_weight, readout.reshape(1, c), energy_offset.reshape(1, ns),
    )
    forces = forces[:, : 3 * slots].reshape(X, Y, Z, 3, slots)
    return energy.reshape(X, Y, Z, slots), jnp.swapaxes(forces, -1, -2)


def solution(mesh):
    g = P("gx", "gy", "gz")
    return jax.shard_map(
        shards,
        mesh=mesh,
        in_specs=(g, g, g, g, P(), P(), P(), P(), P()),
        out_specs=(g, g),
        check_vma=False,
    )
```

```python
import functools
import itertools
import math

import jax
import jax.numpy as jnp
from jax import lax
from jax.experimental import pallas as pl
from jax.experimental.pallas import tpu as pltpu
from jax.sharding import PartitionSpec as P

F32 = jnp.float32
BF16 = jnp.bfloat16
MESH = pl.DeviceIdType.MESH
AXES = ("gx", "gy", "gz")
RC = 2.0
NO_EDGE = 256
OFFSETS = [o for o in itertools.product((-1, 0, 1), repeat=3) if any(o)]
ORDERS = ((0, 1), (1, 4), (4, 9))
VM = pl.BlockSpec(memory_space=pltpu.VMEM)

NN = ((1,), (0,))
NT = ((1,), (1,))
TN = ((0,), (0,))


def split(x):
    hi = x.astype(BF16)
    return hi, (x - hi.astype(F32)).astype(BF16)


def split32(x):
    hi = x.astype(BF16).astype(F32)
    return hi, x - hi


def mm(a, b, dims):
    return lax.dot_general(a, b, (dims, ((), ())), preferred_element_type=F32)


def mm3(a, b, dims):
    return mm(a[0], b[0], dims) + (mm(a[0], b[1], dims) + mm(a[1], b[0], dims))


def peer(o):
    ids = []
    for axis, step in zip(AXES, o):
        n = lax.axis_size(axis)
        ids.append(lax.rem(lax.axis_index(axis) + (step + n), n))
    return tuple(ids)


def greet():
    barrier = pltpu.get_barrier_semaphore()
    for o in OFFSETS:
        pl.semaphore_signal(barrier, inc=1, device_id=peer(o), device_id_type=MESH)
    pl.semaphore_wait(barrier, len(OFFSETS))


def box(o, dims, minus, zero, plus):
    out = []
    for s, n in zip(o, dims):
        out.append(zero(n) if s == 0 else (plus(n) if s > 0 else minus(n)))
    return tuple(out)


def face(o, dims):
    return box(o, dims, lambda n: pl.ds(0, 1), lambda n: pl.ds(0, n), lambda n: pl.ds(n - 1, 1))


def halo(o, dims):
    return box(o, dims, lambda n: pl.ds(0, 1), lambda n: pl.ds(1, n), lambda n: pl.ds(n + 1, 1))


def opposite(o):
    return tuple(-s for s in o)


def iota(shape, dim):
    return lax.broadcasted_iota(jnp.int32, shape, dim)


def slot_mask(slots, lanes):
    per = lanes // slots
    lane, row = iota((slots, lanes), 1), iota((slots, lanes), 0)
    return jnp.where((lane >= row * per) & (lane < row * per + per), 1.0, 0.0).astype(F32)


def basis(geom, nb):
    dx, dy, dz, ms = geom[0:1], geom[1:2], geom[2:3], geom[4:5]
    r2 = dx * dx + dy * dy + dz * dz
    r = jnp.sqrt(r2)
    inside = r < RC
    w = 1.0 - r2 * (1.0 / RC**2)
    u = jnp.where(inside, w * w, 0.0)
    mu = iota((nb, geom.shape[1]), 0).astype(F32) * (RC / (nb - 1))
    g = ((nb - 1) / RC) ** 2
    off = r - mu
    gauss = jnp.exp(-g * off * off)
    rb = gauss * u
    px, py, pz = dx / RC, dy / RC, dz / RC
    c3, c5, c15 = math.sqrt(3.0), math.sqrt(5.0), math.sqrt(15.0)
    ys = [
        ms,
        ms * (c3 * px),
        ms * (c3 * py),
        ms * (c3 * pz),
        ms * (c15 * px * py),
        ms * (c15 * py * pz),
        ms * ((0.5 * c5) * (3.0 * pz * pz - (px * px + py * py + pz * pz))),
        ms * (c15 * px * pz),
        ms * ((0.5 * c15) * (px * px - py * py)),
    ]
    return rb, ys, (r, w, inside, gauss, off, g, (px, py, pz))


def geom_pull(geom, extra, d_rb, d_y):
    r, w, inside, gauss, off, g, (px, py, pz) = extra
    ms = geom[4:5]
    du = jnp.where(inside, -r * w, 0.0)
    u = jnp.where(inside, w * w, 0.0)
    d_r = jnp.sum(d_rb * gauss * (du - 2.0 * g * off * u), 0, keepdims=True)
    c3, c5, c15 = math.sqrt(3.0), math.sqrt(5.0), math.sqrt(15.0)
    gy = [ms * d_y[m : m + 1] for m in range(9)]
    vx = c3 * gy[1] + c15 * (py * gy[4] + pz * gy[7] + px * gy[8]) - c5 * px * gy[6]
    vy = c3 * gy[2] + c15 * (px * gy[4] + pz * gy[5] - py * gy[8]) - c5 * py * gy[6]
    vz = c3 * gy[3] + c15 * (py * gy[5] + px * gy[7]) + 2.0 * c5 * pz * gy[6]
    k = d_r / jnp.maximum(r, 1e-20)
    return [v / RC + k * geom[i : i + 1] for i, v in enumerate((vx, vy, vz))]


def stack3(x, order):
    hi, lo = split32(x)
    parts = {"h": hi, "l": lo}
    rows = [parts[o] for o in order]
    pad = -(3 * x.shape[0]) % 16
    if pad:
        rows.append(jnp.zeros((pad,) + x.shape[1:], F32))
    return jnp.concatenate(rows, 0).astype(BF16)


def invariants_of(a_ref):
    a0 = a_ref[0]
    v = a_ref[1] * a_ref[1] + a_ref[2] * a_ref[2] + a_ref[3] * a_ref[3]
    t = a_ref[4] * a_ref[4]
    for m in range(5, 9):
        t = t + a_ref[m] * a_ref[m]
    return jnp.concatenate([a0, v, t], 1)


def a_grads(a_ref, d_update, mix, g_ref):
    c = d_update.shape[1]
    d_inv = mm3(split(d_update), split(mix), NT)
    for q, (lo, hi) in enumerate(ORDERS):
        part = d_inv[:, q * c : (q + 1) * c]
        for m in range(lo, hi):
            g_ref[m] = part if q == 0 else (2.0 * part) * a_ref[m]


def stencil_of(n):
    cell = n >> 3
    ox = ((cell * 57) >> 9) - 1
    row = (cell * 43) >> 7
    oy = row - 3 * (ox + 1) - 1
    oz = cell - 3 * row - 1
    return ox, oy, oz, n & 7


def ext_hot(n, rows, base, ye, ze):
    ox, oy, oz, slot = stencil_of(n)
    at = jnp.where(n < NO_EDGE, base + (ox * ye + oy) * ze + oz, -1)
    hot = jnp.where(iota((rows, n.shape[1]), 0) == at, 1.0, 0.0)
    return hot, slot


def expand_mat(slots, lanes):
    per = lanes // slots
    row, col = iota((lanes, 3 * lanes), 0), iota((lanes, 3 * lanes), 1)
    return jnp.where((col >= row * per) & (col < row * per + per), 1.0, 0.0).astype(F32)


def silu_parts(v):
    sig = 1.0 / (1.0 + jnp.exp(-v))
    return v * sig, sig * (1.0 + v * (1.0 - sig))


def hot_rows(n, rows):
    return jnp.where(iota((rows, n.shape[1]), 0) == n, 1.0, 0.0).astype(BF16)


def radial_of(rb, w_stack):
    return mm(stack3(rb, "hhl"), w_stack, TN)


def rows_hl(x):
    hi, lo = split32(x)
    return jnp.concatenate([hi, lo], 0).astype(BF16)


def order_rows(ys, mask, q):
    lo, hi = ORDERS[q]
    return jnp.concatenate([ys[m] * mask for m in range(lo, hi)], 0)


def exchange(src, dst, src_at, dst_at, send_sem, recv_sem, base):
    copies = []
    for i, o in enumerate(OFFSETS):
        copies.append(
            pltpu.make_async_remote_copy(
                src_ref=src.at[src_at(o)],
                dst_ref=dst.at[dst_at(o)],
                send_sem=send_sem.at[base + i],
                recv_sem=recv_sem.at[base + i],
                device_id=peer(o),
                device_id_type=MESH,
            )
        )
        copies[-1].start()
    return copies


def kernel(dims, slots, edges, nb, pos_ref, sp_ref, nb_ref, em_ref, emb_ref, w_ref, mix_ref, read_ref,
           off_ref, energy_ref, out_ref,
           own5_ref, own_ref, nbr_ref, spec_ref, force_ref,
           tab_ext, tab2, own_pos, hot_ref, hotx_ref, geom_ref, ym_ref, we_ref, v_ref, a_ref, g_ref,
           dsilu_ref, hid_own, hid_ext, rad_ref, h_ref, t_ref, z_ref, dext, drecv, drb_ref, dy_ref,
           dh_ref, eg_ref, sent, sent5, srecv, fold5, send_sem, recv_sem, local_sem):
    X, Y, Z = dims
    cells = X * Y * Z
    atoms = cells * slots
    ye, ze = Y + 2, Z + 2
    rows = (X + 2) * ye * ze
    lanes = slots * edges
    c = mix_ref.shape[-1]
    ns = emb_ref.shape[0]
    near = 27 * slots
    near_pad = hot_ref.shape[1]
    n_o = len(OFFSETS)
    s = edges ** (-0.5)
    mask = slot_mask(slots, lanes)
    own_face = lambda o: face(o, dims)
    own_in = lambda o: halo(opposite(o), dims)
    ext_face = lambda o: halo(o, dims)
    inner = tuple(pl.ds(1, n) for n in dims)
    grid = list(itertools.product(*[range(d + 2) for d in dims]))

    barrier = pltpu.get_barrier_semaphore()
    for o in OFFSETS:
        pl.semaphore_signal(barrier, inc=1, device_id=peer(o), device_id_type=MESH)

    def base_of(cx, cy, cz):
        return ((cx + 1) * ye + cy + 1) * ze + cz + 1

    def loop(body):
        def step(i, carry):
            cx, cy = i // Y, i % Y
            body(i, cx, cy)
            return carry
        lax.fori_loop(0, X * Y, step, 0)

    def edge_rows(cell):
        return pl.ds(pl.multiple_of(cell * lanes, lanes), lanes)

    def atom_rows(cell):
        return pl.ds(pl.multiple_of(cell * slots, slots), slots)

    def build_hot(i, cx, cy):
        for cz in range(Z):
            cell = i * Z + cz
            n = nbr_ref[pl.ds(cell, 1), :]
            hot_ref[cell] = hot_rows(n, near_pad)
            hotx_ref[cell] = ext_hot(n, rows, base_of(cx, cy, cz), ye, ze)[0].astype(BF16)

    own_ref[...] = jnp.zeros_like(own_ref)
    for i in range(X * Y):
        cx, cy = i // Y, i % Y
        block = pl.ds(i * Z, Z)
        for k in range(3):
            own_ref[block, k * slots : (k + 1) * slots] = pos_ref[cx, cy, k]
        own_ref[block, 3 * slots : 4 * slots] = sp_ref[cx, cy].astype(F32)
        for cz in range(Z):
            cell = i * Z + cz
            spec_ref[0:1, cell * slots : (cell + 1) * slots] = sp_ref[cx, cy, cz : cz + 1, :]
            own5_ref[cx, cy, cz] = own_ref[cell : cell + 1, :]
    coded = jnp.where(em_ref[...] != 0, nb_ref[...], NO_EDGE).reshape(atoms, edges).astype(F32)
    lane = iota((edges, lanes), 1)
    repeat = jnp.where((lane & (edges - 1)) == iota((edges, lanes), 0), 1.0, 0.0).astype(BF16)
    wide = mm(coded.astype(BF16), repeat, NN).reshape(cells, slots, lanes)
    nbr_ref[...] = jnp.sum(wide * mask[None], 1).astype(jnp.int32)
    loop(build_hot)
    pl.semaphore_wait(barrier, n_o)

    local = pltpu.make_async_copy(own5_ref, tab_ext.at[inner], local_sem.at[0])
    local.start()
    copies = exchange(own5_ref, tab_ext, own_face, own_in, send_sem, recv_sem, 0)
    own_pos[...] = lax.dot_general(
        own_ref[...], expand_mat(slots, lanes), (NN, ((), ())),
        precision=lax.Precision.HIGHEST, preferred_element_type=F32,
    )
    emb = emb_ref[...]
    for k in range(ns):
        wide = jnp.concatenate([emb[k : k + 1]] * 3, 1)
        we_ref[k * nb : (k + 1) * nb, :] = w_ref[0] * wide
    spec_row = spec_ref[...]
    spec_hot = jnp.where(iota((16, atoms), 0) == spec_row, 1.0, 0.0).astype(BF16)
    emb_hi, emb_lo = split(jnp.concatenate([emb, jnp.zeros((16 - ns, c), F32)], 0))
    h0 = mm(spec_hot, emb_hi, TN) + mm(spec_hot, emb_lo, TN)
    eye = jnp.where(iota((4 * slots, lanes), 0) == iota((4 * slots, lanes), 1), 1.0, 0.0).astype(BF16)
    local.wait()
    for copy in copies:
        copy.wait()

    for r, at in enumerate(grid):
        tab2[r : r + 1, :] = tab_ext[at]
    tab = tab2[...]
    hi, rest = split32(tab)
    mid, low = split32(rest)
    tab_t = jnp.concatenate([mm(eye, p.astype(BF16), NT) for p in (hi, mid, low)], 0).astype(BF16)

    def rb_species(rb, geom):
        return jnp.concatenate([jnp.where(geom[3:4] == float(k), rb, 0.0) for k in range(ns)], 0)

    def layer0(i, cx, cy):
        for cz in range(Z):
            cell = i * Z + cz
            n = nbr_ref[pl.ds(cell, 1), :]
            got = mm(tab_t, hotx_ref[cell], NN)
            got = got[: 4 * slots] + got[4 * slots : 8 * slots] + got[8 * slots :]
            ox, oy, oz, slot = stencil_of(n)
            pick = iota((slots, lanes), 0) == slot
            vals = [
                jnp.sum(jnp.where(pick, got[k * slots : (k + 1) * slots], 0.0), 0, keepdims=True)
                for k in range(4)
            ]
            mine = own_pos[pl.ds(cell, 1), :]
            disp = [
                o.astype(F32) + vals[k] - mine[:, k * lanes : (k + 1) * lanes]
                for k, o in enumerate((ox, oy, oz))
            ]
            ms = jnp.where(n < NO_EDGE, s, 0.0)
            zero = jnp.zeros_like(ms)
            geom = jnp.concatenate(disp + [vals[3], ms, zero, zero, zero], 0)
            geom_ref[cell] = geom
            rb, ys, _ = basis(geom, nb)
            blocks = [rows_hl(order_rows(ys, mask, q)) for q in range(3)]
            ym = jnp.concatenate(blocks, 0)
            ym_ref[cell] = ym
            rbs = rb_species(rb, geom)
            v = mm(ym, rows_hl(rbs), NT)
            w = ns * nb
            v = v[:, :w] + v[:, w : 2 * w]
            at = 0
            for lo, hi in ORDERS:
                span = (hi - lo) * slots
                part = v[at : at + span] + v[at + span : at + 2 * span]
                at += 2 * span
                for m in range(lo, hi):
                    v_ref[m, atom_rows(cell), :] = part[(m - lo) * slots : (m - lo + 1) * slots]

    loop(layer0)
    for q, (lo, hi) in enumerate(ORDERS):
        part = split(we_ref[:, q * c : (q + 1) * c])
        for m in range(lo, hi):
            a_ref[0, m] = mm3(split(v_ref[m]), part, NN)
    v = mm3(split(invariants_of(a_ref.at[0])), split(mix_ref[0]), NN)
    up, slope = silu_parts(v)
    dsilu_ref[...] = slope
    hid1 = h0 + up
    hid_own[...] = hid1.reshape(X, Y, Z, slots, c)
    local = pltpu.make_async_copy(hid_own, hid_ext.at[inner], local_sem.at[1])
    local.start()
    copies = exchange(hid_own, hid_ext, own_face, own_in, send_sem, recv_sem, n_o)

    w1 = w_ref[1]
    w_stack = stack3(w1, "hlh")

    def radials(i, cx, cy):
        for cz in range(Z):
            cell = i * Z + cz
            rb, _, _ = basis(geom_ref[cell], nb)
            rad_ref[edge_rows(cell), :] = radial_of(rb, w_stack)

    loop(radials)
    local.wait()
    for copy in copies:
        copy.wait()

    def layer1(i, cx, cy):
        for cz in range(Z):
            cell = i * Z + cz
            table = jnp.concatenate(
                [
                    hid_ext[cx + a, cy + b, pl.ds(cz, 3)].reshape(3 * slots, c)
                    for a in range(3)
                    for b in range(3)
                ]
                + [jnp.zeros((near_pad - near, c), F32)],
                0,
            )
            both = mm(hot_ref[cell], jnp.concatenate(split(table), 1), TN)
            h = both[:, :c] + both[:, c:]
            h_ref[edge_rows(cell), :] = h
            ym = ym_ref[cell]
            at = 0
            for q, (lo, hi) in enumerate(ORDERS):
                t = rad_ref[edge_rows(cell), q * c : (q + 1) * c] * h
                t_hi, t_lo = split(t)
                t_ref[cell, q, :lanes, :] = t_hi
                t_ref[cell, q, lanes:, :] = t_lo
                span = (hi - lo) * slots
                sums = mm(ym[at : at + 2 * span], jnp.concatenate([t_hi, t_lo], 1), NN)
                at += 2 * span
                sums = sums[:, :c] + sums[:, c:]
                sums = sums[:span] + sums[span:]
                for m in range(lo, hi):
                    a_ref[1, m, atom_rows(cell), :] = sums[(m - lo) * slots : (m - lo + 1) * slots]

    loop(layer1)
    read = read_ref[...]
    v = mm3(split(invariants_of(a_ref.at[1])), split(mix_ref[1]), NN)
    up, slope = silu_parts(v)
    a_grads(a_ref.at[1], slope * read, mix_ref[1], g_ref)
    dext[...] = jnp.zeros_like(dext)

    def back1(i, cx, cy):
        for cz in range(Z):
            cell = i * Z + cz
            h = h_ref[edge_rows(cell), :]
            ym = ym_ref[cell]
            d_h = None
            at = 0
            for q, (lo, hi) in enumerate(ORDERS):
                span = (hi - lo) * slots
                grads = jnp.concatenate([g_ref[m, atom_rows(cell), :] for m in range(lo, hi)], 0)
                g_hi, g_lo = split32(grads)
                yq = ym[at : at + 2 * span]
                at += 2 * span
                lhs = jnp.concatenate([yq, yq], 0)
                rhs = jnp.concatenate([g_hi, g_hi, g_lo, g_lo], 0).astype(BF16)
                pull = mm(lhs, rhs, TN)
                term = pull * rad_ref[edge_rows(cell), q * c : (q + 1) * c]
                d_h = term if d_h is None else d_h + term
                z_hi, z_lo = split(pull * h)
                z_ref[cell, :lanes, q * c : (q + 1) * c] = z_hi
                z_ref[cell, lanes:, q * c : (q + 1) * c] = z_lo
            both = mm(hot_ref[cell], jnp.concatenate(split(d_h), 1), NN)
            sums = both[:, :c] + both[:, c:]
            for j, (a, b) in enumerate(itertools.product(range(3), repeat=2)):
                at = (cx + a, cy + b, pl.ds(cz, 3))
                part = sums[j * 3 * slots : (j + 1) * 3 * slots].reshape(3, slots, c)
                dext[at] = dext[at] + part

    loop(back1)
    copies = exchange(dext, drecv, ext_face, ext_face, send_sem, recv_sem, 2 * n_o)

    hid2 = hid_ext[1 : X + 1, 1 : Y + 1, 1 : Z + 1].reshape(atoms, c) + up
    read8 = jnp.concatenate([read] * 8, 0)
    energy = mm3(split(read8), split(hid2), NT)[0:1]
    for k in range(ns):
        energy = energy + jnp.where(spec_row == k, off_ref[k], 0.0)
    for r, (cx, cy, cz) in enumerate(itertools.product(*[range(d) for d in dims])):
        energy_ref[cx, cy, cz : cz + 1, :] = energy[:, r * slots : (r + 1) * slots]
    w_rows = rows_hl(w1)

    def pull_rows(full, first, count):
        return [
            jnp.sum(full[m * slots : (m + 1) * slots] * mask, 0, keepdims=True)
            for m in range(first, first + count)
        ]

    def geom1(i, cx, cy):
        for cz in range(Z):
            cell = i * Z + cz
            d = mm(w_rows, z_ref[cell], NT)
            d = d[:, :lanes] + d[:, lanes:]
            drb_ref[cell] = d[:nb] + d[nb:]
            d_y = [jnp.zeros((1, lanes), F32)]
            for q in (1, 2):
                lo, hi = ORDERS[q]
                grads = jnp.concatenate([g_ref[m, atom_rows(cell), :] for m in range(lo, hi)], 0)
                full = mm(rows_hl(grads), t_ref[cell, q], NT)
                full = full[:, :lanes] + full[:, lanes:]
                span = (hi - lo) * slots
                d_y += pull_rows(full[:span] + full[span:], 0, hi - lo)
            dy_ref[cell] = jnp.concatenate(d_y + [d_y[0]] * 7, 0)

    loop(geom1)
    dh_ref[...] = dext[inner]
    for o, copy in zip(OFFSETS, copies):
        copy.wait()
        at = face(opposite(o), dims)
        dh_ref[at] = dh_ref[at] + drecv[halo(o, dims)]

    cot = dh_ref[...].reshape(atoms, c) + read
    a_grads(a_ref.at[0], dsilu_ref[...] * cot, mix_ref[0], g_ref)
    for q, (lo, hi) in enumerate(ORDERS):
        part = split(we_ref[:, q * c : (q + 1) * c])
        for m in range(lo, hi):
            v_ref[m] = mm3(split(g_ref[m]), part, NT)
    sent[...] = jnp.zeros_like(sent)

    def back0(i, cx, cy):
        hots, xs = [], []
        for cz in range(Z):
            cell = i * Z + cz
            geom = geom_ref[cell]
            rb, ys, extra = basis(geom, nb)
            rbs = rb_species(rb, geom)
            d_v = jnp.concatenate([v_ref[m, atom_rows(cell), :] for m in range(9)], 0)
            d_v = split32(d_v)
            r_v = split32(rbs)
            lhs = jnp.concatenate([d_v[0], d_v[1]], 0).astype(BF16)
            rhs = jnp.concatenate([r_v[0], r_v[1]], 1).astype(BF16)
            full = mm(lhs, rhs, NN)
            full = full[:, :lanes] + full[:, lanes:]
            full = full[: 9 * slots] + full[9 * slots :]
            d_y = [jnp.zeros((1, lanes), F32)] + pull_rows(full, 1, 8)
            yall = jnp.concatenate([y * mask for y in ys], 0)
            d_rbs = mm(
                jnp.concatenate([d_v[0], d_v[0], d_v[1], jnp.zeros((slots, ns * nb), F32)], 0).astype(BF16),
                stack3(yall, "hlh"),
                TN,
            )
            d_rb = drb_ref[cell]
            for k in range(ns):
                d_rb = d_rb + jnp.where(geom[3:4] == float(k), d_rbs[k * nb : (k + 1) * nb], 0.0)
            d_y = jnp.concatenate(d_y + [d_y[0]] * 7, 0) + dy_ref[cell]
            grads = geom_pull(geom, extra, d_rb, d_y)
            eg_ref[pl.ds(cell, 1), :] = jnp.concatenate(grads, 1)
            slot = stencil_of(nbr_ref[pl.ds(cell, 1), :])[3]
            pick = iota((slots, lanes), 0) == slot
            zero = jnp.zeros((slots, lanes), F32)
            x_hi, x_lo = split32(jnp.concatenate([jnp.where(pick, g, 0.0) for g in grads] + [zero], 0))
            hot = hotx_ref[cell]
            hots += [hot, hot]
            xs += [x_hi.astype(BF16), x_lo.astype(BF16)]
        sent[...] += mm(jnp.concatenate(hots, 1), jnp.concatenate(xs, 1), NT)

    loop(back0)
    sent5[...] = jnp.zeros_like(sent5)
    width = sent.shape[1]
    for r, at in enumerate(grid):
        sent5[at + (slice(None), slice(0, width))] = sent[r : r + 1, :]
    copies = exchange(sent5, srecv, ext_face, ext_face, send_sem, recv_sem, 3 * n_o)
    force_ref[...] = lax.dot_general(
        eg_ref[...], expand_mat(slots, lanes), (NT, ((), ())),
        precision=lax.Precision.HIGHEST, preferred_element_type=F32,
    )
    fold5[...] = sent5[inner]
    for o, copy in zip(OFFSETS, copies):
        copy.wait()
        at = face(opposite(o), dims)
        fold5[at] = fold5[at] + srecv[halo(o, dims)]
    for r, at in enumerate(itertools.product(*[range(d) for d in dims])):
        force_ref[r : r + 1, :] = force_ref[r : r + 1, :] - fold5[at]
    for i in range(X * Y):
        for k in range(3):
            out_ref[i // Y, i % Y, k] = force_ref[pl.ds(i * Z, Z), k * slots : (k + 1) * slots]


def shards(positions, species, neighbors, edge_mask, species_embed, radial_weight, mix_weight, readout, energy_offset):
    X, Y, Z, slots, edges = neighbors.shape
    dims = (X, Y, Z)
    cells = X * Y * Z
    atoms = cells * slots
    lanes = slots * edges
    ns, c = species_embed.shape
    nb = radial_weight.shape[1]
    ext = (X + 2, Y + 2, Z + 2)
    rows = ext[0] * ext[1] * ext[2]
    near = -(-27 * slots // 256) * 256

    vm = pltpu.VMEM
    count = 4 * len(OFFSETS)
    smem = pl.BlockSpec(memory_space=pltpu.SMEM)
    energy, forces = pl.pallas_call(
        functools.partial(kernel, dims, slots, edges, nb),
        out_shape=[
            jax.ShapeDtypeStruct(dims + (slots,), F32),
            jax.ShapeDtypeStruct((X, Y, 3, Z, slots), F32),
        ],
        in_specs=[VM] * 8 + [smem],
        out_specs=[VM, VM],
        scratch_shapes=[
            vm(dims + (1, lanes), F32),
            vm((cells, lanes), F32),
            vm((cells, lanes), jnp.int32),
            vm((1, atoms), jnp.int32),
            vm((cells, lanes), F32),
            vm(ext + (1, lanes), F32),
            vm((rows, lanes), F32),
            vm((cells, 3 * lanes), F32),
            vm((cells, near, lanes), BF16),
            vm((cells, rows, lanes), BF16),
            vm((cells, 8, lanes), F32),
            vm((cells, 18 * slots, lanes), BF16),
            vm((ns * nb, 3 * c), F32),
            vm((9, atoms, ns * nb), F32),
            vm((2, 9, atoms, c), F32),
            vm((9, atoms, c), F32),
            vm((atoms, c), F32),
            vm(dims + (slots, c), F32),
            vm(ext + (slots, c), F32),
            vm((cells * lanes, 3 * c), F32),
            vm((cells * lanes, c), F32),
            vm((cells, 3, 2 * lanes, c), BF16),
            vm((cells, 2 * lanes, 3 * c), BF16),
            vm(ext + (slots, c), F32),
            vm(ext + (slots, c), F32),
            vm((cells, nb, lanes), F32),
            vm((cells, 16, lanes), F32),
            vm(dims + (slots, c), F32),
            vm((cells, 3 * lanes), F32),
            vm((rows, 4 * slots), F32),
            vm(ext + (1, lanes), F32),
            vm(ext + (1, lanes), F32),
            vm(dims + (1, lanes), F32),
            pltpu.SemaphoreType.DMA((count,)),
            pltpu.SemaphoreType.DMA((count,)),
            pltpu.SemaphoreType.DMA((2,)),
        ],
        compiler_params=pltpu.CompilerParams(
            collective_id=1, has_side_effects=True, vmem_limit_bytes=58 * 1024 * 1024
        ),
        name="potential",
    )(
        jnp.transpose(positions, (0, 1, 4, 2, 3)), species, neighbors, edge_mask, species_embed,
        radial_weight, mix_weight, readout.reshape(1, c), energy_offset,
    )
    return energy, jnp.transpose(forces, (0, 1, 3, 4, 2))


def solution(mesh):
    g = P("gx", "gy", "gz")
    return jax.shard_map(
        shards,
        mesh=mesh,
        in_specs=(g, g, g, g, P(), P(), P(), P(), P()),
        out_specs=(g, g),
        check_vma=False,
    )
```

```python
import functools
import itertools
import math

import jax
import jax.numpy as jnp
from jax import lax
from jax.experimental import pallas as pl
from jax.experimental.pallas import tpu as pltpu
from jax.sharding import PartitionSpec as P

F32 = jnp.float32
BF16 = jnp.bfloat16
MESH = pl.DeviceIdType.MESH
AXES = ("gx", "gy", "gz")
RC = 2.0
NO_EDGE = 256
OFFSETS = sorted((o for o in itertools.product((-1, 0, 1), repeat=3) if any(o)), key=lambda o: -o[0])
ORDERS = ((0, 1), (1, 4), (4, 9))
VM = pl.BlockSpec(memory_space=pltpu.VMEM)

NN = ((1,), (0,))
NT = ((1,), (1,))
TN = ((0,), (0,))


def split(x):
    hi = x.astype(BF16)
    return hi, (x - hi.astype(F32)).astype(BF16)


def split32(x):
    hi = x.astype(BF16).astype(F32)
    return hi, x - hi


def mm(a, b, dims):
    return lax.dot_general(a, b, (dims, ((), ())), preferred_element_type=F32)


def mm3(a, b, dims):
    return mm(a[0], b[0], dims) + (mm(a[0], b[1], dims) + mm(a[1], b[0], dims))


def peer(o):
    ids = []
    for axis, step in zip(AXES, o):
        n = lax.axis_size(axis)
        ids.append(lax.rem(lax.axis_index(axis) + (step + n), n))
    return tuple(ids)


def greet():
    barrier = pltpu.get_barrier_semaphore()
    for o in OFFSETS:
        pl.semaphore_signal(barrier, inc=1, device_id=peer(o), device_id_type=MESH)
    pl.semaphore_wait(barrier, len(OFFSETS))


def box(o, dims, minus, zero, plus):
    out = []
    for s, n in zip(o, dims):
        out.append(zero(n) if s == 0 else (plus(n) if s > 0 else minus(n)))
    return tuple(out)


def face(o, dims):
    return box(o, dims, lambda n: pl.ds(0, 1), lambda n: pl.ds(0, n), lambda n: pl.ds(n - 1, 1))


def halo(o, dims):
    return box(o, dims, lambda n: pl.ds(0, 1), lambda n: pl.ds(1, n), lambda n: pl.ds(n + 1, 1))


def opposite(o):
    return tuple(-s for s in o)


def iota(shape, dim):
    return lax.broadcasted_iota(jnp.int32, shape, dim)


def slot_mask(slots, lanes):
    per = lanes // slots
    lane, row = iota((slots, lanes), 1), iota((slots, lanes), 0)
    return jnp.where((lane >= row * per) & (lane < row * per + per), 1.0, 0.0).astype(F32)


def basis(geom, nb):
    dx, dy, dz, ms = geom[0:1], geom[1:2], geom[2:3], geom[4:5]
    r2 = dx * dx + dy * dy + dz * dz
    r = jnp.sqrt(r2)
    inside = r < RC
    w = 1.0 - r2 * (1.0 / RC**2)
    u = jnp.where(inside, w * w, 0.0)
    mu = iota((nb, geom.shape[1]), 0).astype(F32) * (RC / (nb - 1))
    g = ((nb - 1) / RC) ** 2
    off = r - mu
    gauss = jnp.exp(-g * off * off)
    rb = gauss * u
    px, py, pz = dx / RC, dy / RC, dz / RC
    c3, c5, c15 = math.sqrt(3.0), math.sqrt(5.0), math.sqrt(15.0)
    ys = [
        ms,
        ms * (c3 * px),
        ms * (c3 * py),
        ms * (c3 * pz),
        ms * (c15 * px * py),
        ms * (c15 * py * pz),
        ms * ((0.5 * c5) * (3.0 * pz * pz - (px * px + py * py + pz * pz))),
        ms * (c15 * px * pz),
        ms * ((0.5 * c15) * (px * px - py * py)),
    ]
    return rb, ys, (r, w, inside, gauss, off, g, (px, py, pz))


def geom_pull(geom, extra, d_rb, d_y):
    r, w, inside, gauss, off, g, (px, py, pz) = extra
    ms = geom[4:5]
    du = jnp.where(inside, -r * w, 0.0)
    u = jnp.where(inside, w * w, 0.0)
    d_r = jnp.sum(d_rb * gauss * (du - 2.0 * g * off * u), 0, keepdims=True)
    c3, c5, c15 = math.sqrt(3.0), math.sqrt(5.0), math.sqrt(15.0)
    gy = [ms * d_y[m : m + 1] for m in range(9)]
    vx = c3 * gy[1] + c15 * (py * gy[4] + pz * gy[7] + px * gy[8]) - c5 * px * gy[6]
    vy = c3 * gy[2] + c15 * (px * gy[4] + pz * gy[5] - py * gy[8]) - c5 * py * gy[6]
    vz = c3 * gy[3] + c15 * (py * gy[5] + px * gy[7]) + 2.0 * c5 * pz * gy[6]
    k = d_r / jnp.maximum(r, 1e-20)
    return [v / RC + k * geom[i : i + 1] for i, v in enumerate((vx, vy, vz))]


def stack3(x, order):
    hi, lo = split32(x)
    parts = {"h": hi, "l": lo}
    rows = [parts[o] for o in order]
    pad = -(3 * x.shape[0]) % 16
    if pad:
        rows.append(jnp.zeros((pad,) + x.shape[1:], F32))
    return jnp.concatenate(rows, 0).astype(BF16)


def invariants_of(a_ref):
    a0 = a_ref[0]
    v = a_ref[1] * a_ref[1] + a_ref[2] * a_ref[2] + a_ref[3] * a_ref[3]
    t = a_ref[4] * a_ref[4]
    for m in range(5, 9):
        t = t + a_ref[m] * a_ref[m]
    return jnp.concatenate([a0, v, t], 1)


def a_grads(a_ref, d_update, mix, g_ref):
    c = d_update.shape[1]
    d_inv = mm3(split(d_update), split(mix), NT)
    for q, (lo, hi) in enumerate(ORDERS):
        part = d_inv[:, q * c : (q + 1) * c]
        for m in range(lo, hi):
            g_ref[m] = part if q == 0 else (2.0 * part) * a_ref[m]


def stencil_of(n):
    cell = n >> 3
    ox = ((cell * 57) >> 9) - 1
    row = (cell * 43) >> 7
    oy = row - 3 * (ox + 1) - 1
    oz = cell - 3 * row - 1
    return ox, oy, oz, n & 7


def ext_hot(n, rows, base, ye, ze):
    ox, oy, oz, slot = stencil_of(n)
    at = jnp.where(n < NO_EDGE, base + (ox * ye + oy) * ze + oz, -1)
    hot = jnp.where(iota((rows, n.shape[1]), 0) == at, 1.0, 0.0)
    return hot, slot


def expand_mat(slots, lanes):
    per = lanes // slots
    row, col = iota((lanes, 3 * lanes), 0), iota((lanes, 3 * lanes), 1)
    return jnp.where((col >= row * per) & (col < row * per + per), 1.0, 0.0).astype(F32)


def silu_parts(v):
    sig = 1.0 / (1.0 + jnp.exp(-v))
    return v * sig, sig * (1.0 + v * (1.0 - sig))


def hot_rows(n, rows):
    return jnp.where(iota((rows, n.shape[1]), 0) == n, 1.0, 0.0).astype(BF16)


def radial_of(rb, w_stack):
    return mm(stack3(rb, "hhl"), w_stack, TN)


def rows_hl(x):
    hi, lo = split32(x)
    return jnp.concatenate([hi, lo], 0).astype(BF16)


def order_rows(ys, mask, q):
    lo, hi = ORDERS[q]
    return jnp.concatenate([ys[m] * mask for m in range(lo, hi)], 0)


def exchange(src, dst, src_at, dst_at, send_sem, recv_sem, base, only=(-1, 0, 1)):
    copies = []
    for i, o in enumerate(OFFSETS):
        if o[0] not in only:
            continue
        copies.append(
            pltpu.make_async_remote_copy(
                src_ref=src.at[src_at(o)],
                dst_ref=dst.at[dst_at(o)],
                send_sem=send_sem.at[base + i],
                recv_sem=recv_sem.at[base + i],
                device_id=peer(o),
                device_id_type=MESH,
            )
        )
        copies[-1].start()
    return copies


def kernel(dims, slots, edges, nb, pos_ref, sp_ref, nb_ref, em_ref, emb_ref, w_ref, mix_ref, read_ref,
           off_ref, out_ref,
           own5_ref, own_ref, nbr_ref, spec_ref, force_ref,
           tab_ext, tab2, own_pos, hot_ref, hotx_ref, geom_ref, ym_ref, we_ref, v_ref, a_ref, g_ref,
           dsilu_ref, hid_own, hid_ext, rad_ref, h_ref, t_ref, z_ref, dext, drecv, drb_ref, dy_ref,
           dh_ref, eg_ref, sent, sent5, srecv, fold5, send_sem, recv_sem, local_sem):
    X, Y, Z = dims
    cells = X * Y * Z
    atoms = cells * slots
    ye, ze = Y + 2, Z + 2
    rows = (X + 2) * ye * ze
    lanes = slots * edges
    c = mix_ref.shape[-1]
    ns = emb_ref.shape[0]
    near = 27 * slots
    near_pad = hot_ref.shape[1]
    n_o = len(OFFSETS)
    s = edges ** (-0.5)
    mask = slot_mask(slots, lanes)
    own_face = lambda o: face(o, dims)
    own_in = lambda o: halo(opposite(o), dims)
    ext_face = lambda o: halo(o, dims)
    inner = tuple(pl.ds(1, n) for n in dims)
    grid = list(itertools.product(*[range(d + 2) for d in dims]))

    barrier = pltpu.get_barrier_semaphore()
    for o in OFFSETS:
        pl.semaphore_signal(barrier, inc=1, device_id=peer(o), device_id_type=MESH)

    def base_of(cx, cy, cz):
        return ((cx + 1) * ye + cy + 1) * ze + cz + 1

    def loop(body, first=0, last=X * Y):
        def step(i, carry):
            cx, cy = i // Y, i % Y
            body(i, cx, cy)
            return carry
        lax.fori_loop(first, last, step, 0)

    def edge_rows(cell):
        return pl.ds(pl.multiple_of(cell * lanes, lanes), lanes)

    def atom_rows(cell):
        return pl.ds(pl.multiple_of(cell * slots, slots), slots)

    def build_hot(i, cx, cy):
        for cz in range(Z):
            cell = i * Z + cz
            n = nbr_ref[pl.ds(cell, 1), :]
            hot_ref[cell] = hot_rows(n, near_pad)
            hotx_ref[cell] = ext_hot(n, rows, base_of(cx, cy, cz), ye, ze)[0].astype(BF16)

    own_ref[...] = jnp.zeros_like(own_ref)
    for i in range(X * Y):
        cx, cy = i // Y, i % Y
        block = pl.ds(i * Z, Z)
        for k in range(3):
            own_ref[block, k * slots : (k + 1) * slots] = pos_ref[cx, cy, k]
        own_ref[block, 3 * slots : 4 * slots] = sp_ref[cx, cy].astype(F32)
        for cz in range(Z):
            cell = i * Z + cz
            spec_ref[0:1, cell * slots : (cell + 1) * slots] = sp_ref[cx, cy, cz : cz + 1, :]
            own5_ref[cx, cy, cz] = own_ref[cell : cell + 1, :]
    coded = jnp.where(em_ref[...] != 0, nb_ref[...], NO_EDGE).reshape(atoms, edges).astype(F32)
    lane = iota((edges, lanes), 1)
    repeat = jnp.where((lane & (edges - 1)) == iota((edges, lanes), 0), 1.0, 0.0).astype(BF16)
    wide = mm(coded.astype(BF16), repeat, NN).reshape(cells, slots, lanes)
    nbr_ref[...] = jnp.sum(wide * mask[None], 1).astype(jnp.int32)
    loop(build_hot)
    pl.semaphore_wait(barrier, n_o)

    local = pltpu.make_async_copy(own5_ref, tab_ext.at[inner], local_sem.at[0])
    local.start()
    copies = exchange(own5_ref, tab_ext, own_face, own_in, send_sem, recv_sem, 0)
    own_pos[...] = lax.dot_general(
        own_ref[...], expand_mat(slots, lanes), (NN, ((), ())),
        precision=lax.Precision.HIGHEST, preferred_element_type=F32,
    )
    emb = emb_ref[...]
    for k in range(ns):
        wide = jnp.concatenate([emb[k : k + 1]] * 3, 1)
        we_ref[k * nb : (k + 1) * nb, :] = w_ref[0] * wide
    spec_row = spec_ref[...]
    spec_hot = jnp.where(iota((16, atoms), 0) == spec_row, 1.0, 0.0).astype(BF16)
    emb_hi, emb_lo = split(jnp.concatenate([emb, jnp.zeros((16 - ns, c), F32)], 0))
    h0 = mm(spec_hot, emb_hi, TN) + mm(spec_hot, emb_lo, TN)
    eye = jnp.where(iota((4 * slots, lanes), 0) == iota((4 * slots, lanes), 1), 1.0, 0.0).astype(BF16)
    local.wait()
    for copy in copies:
        copy.wait()

    for r, at in enumerate(grid):
        tab2[r : r + 1, :] = tab_ext[at]
    tab = tab2[...]
    hi, rest = split32(tab)
    mid, low = split32(rest)
    tab_t = jnp.concatenate([mm(eye, p.astype(BF16), NT) for p in (hi, mid, low)], 0).astype(BF16)

    def rb_species(rb, geom):
        return jnp.concatenate([jnp.where(geom[3:4] == float(k), rb, 0.0) for k in range(ns)], 0)

    def layer0(i, cx, cy):
        for cz in range(Z):
            cell = i * Z + cz
            n = nbr_ref[pl.ds(cell, 1), :]
            got = mm(tab_t, hotx_ref[cell], NN)
            got = got[: 4 * slots] + got[4 * slots : 8 * slots] + got[8 * slots :]
            ox, oy, oz, slot = stencil_of(n)
            pick = iota((slots, lanes), 0) == slot
            vals = [
                jnp.sum(jnp.where(pick, got[k * slots : (k + 1) * slots], 0.0), 0, keepdims=True)
                for k in range(4)
            ]
            mine = own_pos[pl.ds(cell, 1), :]
            disp = [
                o.astype(F32) + vals[k] - mine[:, k * lanes : (k + 1) * lanes]
                for k, o in enumerate((ox, oy, oz))
            ]
            ms = jnp.where(n < NO_EDGE, s, 0.0)
            zero = jnp.zeros_like(ms)
            geom = jnp.concatenate(disp + [vals[3], ms, zero, zero, zero], 0)
            geom_ref[cell] = geom
            rb, ys, _ = basis(geom, nb)
            blocks = [rows_hl(order_rows(ys, mask, q)) for q in range(3)]
            ym = jnp.concatenate(blocks, 0)
            ym_ref[cell] = ym
            rbs = rb_species(rb, geom)
            v = mm(ym, rows_hl(rbs), NT)
            w = ns * nb
            v = v[:, :w] + v[:, w : 2 * w]
            at = 0
            for lo, hi in ORDERS:
                span = (hi - lo) * slots
                part = v[at : at + span] + v[at + span : at + 2 * span]
                at += 2 * span
                for m in range(lo, hi):
                    v_ref[m, atom_rows(cell), :] = part[(m - lo) * slots : (m - lo + 1) * slots]

    loop(layer0)
    for q, (lo, hi) in enumerate(ORDERS):
        part = split(we_ref[:, q * c : (q + 1) * c])
        for m in range(lo, hi):
            a_ref[0, m] = mm3(split(v_ref[m]), part, NN)
    v = mm3(split(invariants_of(a_ref.at[0])), split(mix_ref[0]), NN)
    up, slope = silu_parts(v)
    dsilu_ref[...] = slope
    hid1 = h0 + up
    hid_own[...] = hid1.reshape(X, Y, Z, slots, c)
    local = pltpu.make_async_copy(hid_own, hid_ext.at[inner], local_sem.at[1])
    local.start()
    copies = exchange(hid_own, hid_ext, own_face, own_in, send_sem, recv_sem, n_o)

    w1 = w_ref[1]
    w_stack = stack3(w1, "hlh")

    def radials(i, cx, cy):
        for cz in range(Z):
            cell = i * Z + cz
            rb, _, _ = basis(geom_ref[cell], nb)
            rad_ref[edge_rows(cell), :] = radial_of(rb, w_stack)

    loop(radials)
    local.wait()
    late = sum(o[0] == -1 for o in OFFSETS)
    for copy in copies[:-late]:
        copy.wait()

    def layer1(i, cx, cy):
        for cz in range(Z):
            cell = i * Z + cz
            table = jnp.concatenate(
                [
                    hid_ext[cx + a, cy + b, pl.ds(cz, 3)].reshape(3 * slots, c)
                    for a in range(3)
                    for b in range(3)
                ]
                + [jnp.zeros((near_pad - near, c), F32)],
                0,
            )
            both = mm(hot_ref[cell], jnp.concatenate(split(table), 1), TN)
            h = both[:, :c] + both[:, c:]
            h_ref[edge_rows(cell), :] = h
            ym = ym_ref[cell]
            at = 0
            for q, (lo, hi) in enumerate(ORDERS):
                t = rad_ref[edge_rows(cell), q * c : (q + 1) * c] * h
                t_hi, t_lo = split(t)
                t_ref[cell, q, :lanes, :] = t_hi
                t_ref[cell, q, lanes:, :] = t_lo
                span = (hi - lo) * slots
                sums = mm(ym[at : at + 2 * span], jnp.concatenate([t_hi, t_lo], 1), NN)
                at += 2 * span
                sums = sums[:, :c] + sums[:, c:]
                sums = sums[:span] + sums[span:]
                for m in range(lo, hi):
                    a_ref[1, m, atom_rows(cell), :] = sums[(m - lo) * slots : (m - lo + 1) * slots]

    loop(layer1, 0, (X - 1) * Y)
    for copy in copies[-late:]:
        copy.wait()
    loop(layer1, (X - 1) * Y)
    read = read_ref[...]
    v = mm3(split(invariants_of(a_ref.at[1])), split(mix_ref[1]), NN)
    up, slope = silu_parts(v)
    a_grads(a_ref.at[1], slope * read, mix_ref[1], g_ref)
    dext[...] = jnp.zeros_like(dext)

    def back1(i, cx, cy):
        for cz in range(Z):
            cell = i * Z + cz
            h = h_ref[edge_rows(cell), :]
            ym = ym_ref[cell]
            d_h = None
            at = 0
            for q, (lo, hi) in enumerate(ORDERS):
                span = (hi - lo) * slots
                grads = jnp.concatenate([g_ref[m, atom_rows(cell), :] for m in range(lo, hi)], 0)
                g_hi, g_lo = split32(grads)
                yq = ym[at : at + 2 * span]
                at += 2 * span
                lhs = jnp.concatenate([yq, yq], 0)
                rhs = jnp.concatenate([g_hi, g_hi, g_lo, g_lo], 0).astype(BF16)
                pull = mm(lhs, rhs, TN)
                term = pull * rad_ref[edge_rows(cell), q * c : (q + 1) * c]
                d_h = term if d_h is None else d_h + term
                z_hi, z_lo = split(pull * h)
                z_ref[cell, :lanes, q * c : (q + 1) * c] = z_hi
                z_ref[cell, lanes:, q * c : (q + 1) * c] = z_lo
            both = mm(hot_ref[cell], jnp.concatenate(split(d_h), 1), NN)
            sums = both[:, :c] + both[:, c:]
            for j, (a, b) in enumerate(itertools.product(range(3), repeat=2)):
                at = (cx + a, cy + b, pl.ds(cz, 3))
                part = sums[j * 3 * slots : (j + 1) * 3 * slots].reshape(3, slots, c)
                dext[at] = dext[at] + part

    loop(back1, 0, Y)
    early = exchange(dext, drecv, ext_face, ext_face, send_sem, recv_sem, 2 * n_o, (-1,))
    loop(back1, Y)
    copies = exchange(dext, drecv, ext_face, ext_face, send_sem, recv_sem, 2 * n_o, (0, 1)) + early

    hid2 = hid_ext[1 : X + 1, 1 : Y + 1, 1 : Z + 1].reshape(atoms, c) + up
    read8 = jnp.concatenate([read] * 8, 0)
    energy = mm3(split(read8), split(hid2), NT)[0:1]
    for k in range(ns):
        energy = energy + jnp.where(spec_row == k, off_ref[k], 0.0)
    for r, (cx, cy, cz) in enumerate(itertools.product(*[range(d) for d in dims])):
        out_ref[cx, cy, 3, cz : cz + 1, :] = energy[:, r * slots : (r + 1) * slots]
    w_rows = rows_hl(w1)

    def pull_rows(full, first, count):
        return [
            jnp.sum(full[m * slots : (m + 1) * slots] * mask, 0, keepdims=True)
            for m in range(first, first + count)
        ]

    def geom1(i, cx, cy):
        for cz in range(Z):
            cell = i * Z + cz
            d = mm(w_rows, z_ref[cell], NT)
            d = d[:, :lanes] + d[:, lanes:]
            drb_ref[cell] = d[:nb] + d[nb:]
            d_y = [jnp.zeros((1, lanes), F32)]
            for q in (1, 2):
                lo, hi = ORDERS[q]
                grads = jnp.concatenate([g_ref[m, atom_rows(cell), :] for m in range(lo, hi)], 0)
                full = mm(rows_hl(grads), t_ref[cell, q], NT)
                full = full[:, :lanes] + full[:, lanes:]
                span = (hi - lo) * slots
                d_y += pull_rows(full[:span] + full[span:], 0, hi - lo)
            dy_ref[cell] = jnp.concatenate(d_y + [d_y[0]] * 7, 0)

    loop(geom1)
    dh_ref[...] = dext[inner]
    for o, copy in zip(OFFSETS, copies):
        copy.wait()
        at = face(opposite(o), dims)
        dh_ref[at] = dh_ref[at] + drecv[halo(o, dims)]

    cot = dh_ref[...].reshape(atoms, c) + read
    a_grads(a_ref.at[0], dsilu_ref[...] * cot, mix_ref[0], g_ref)
    for q, (lo, hi) in enumerate(ORDERS):
        part = split(we_ref[:, q * c : (q + 1) * c])
        for m in range(lo, hi):
            v_ref[m] = mm3(split(g_ref[m]), part, NT)
    sent[...] = jnp.zeros_like(sent)

    def back0(i, cx, cy):
        hots, xs = [], []
        for cz in range(Z):
            cell = i * Z + cz
            geom = geom_ref[cell]
            rb, ys, extra = basis(geom, nb)
            rbs = rb_species(rb, geom)
            d_v = jnp.concatenate([v_ref[m, atom_rows(cell), :] for m in range(9)], 0)
            d_v = split32(d_v)
            r_v = split32(rbs)
            lhs = jnp.concatenate([d_v[0], d_v[1]], 0).astype(BF16)
            rhs = jnp.concatenate([r_v[0], r_v[1]], 1).astype(BF16)
            full = mm(lhs, rhs, NN)
            full = full[:, :lanes] + full[:, lanes:]
            full = full[: 9 * slots] + full[9 * slots :]
            d_y = [jnp.zeros((1, lanes), F32)] + pull_rows(full, 1, 8)
            yall = jnp.concatenate([y * mask for y in ys], 0)
            d_rbs = mm(
                jnp.concatenate([d_v[0], d_v[0], d_v[1], jnp.zeros((slots, ns * nb), F32)], 0).astype(BF16),
                stack3(yall, "hlh"),
                TN,
            )
            d_rb = drb_ref[cell]
            for k in range(ns):
                d_rb = d_rb + jnp.where(geom[3:4] == float(k), d_rbs[k * nb : (k + 1) * nb], 0.0)
            d_y = jnp.concatenate(d_y + [d_y[0]] * 7, 0) + dy_ref[cell]
            grads = geom_pull(geom, extra, d_rb, d_y)
            eg_ref[pl.ds(cell, 1), :] = jnp.concatenate(grads, 1)
            slot = stencil_of(nbr_ref[pl.ds(cell, 1), :])[3]
            pick = iota((slots, lanes), 0) == slot
            zero = jnp.zeros((slots, lanes), F32)
            x_hi, x_lo = split32(jnp.concatenate([jnp.where(pick, g, 0.0) for g in grads] + [zero], 0))
            hot = hotx_ref[cell]
            hots += [hot, hot]
            xs += [x_hi.astype(BF16), x_lo.astype(BF16)]
        sent[...] += mm(jnp.concatenate(hots, 1), jnp.concatenate(xs, 1), NT)

    loop(back0)
    sent5[...] = jnp.zeros_like(sent5)
    width = sent.shape[1]
    for r, at in enumerate(grid):
        sent5[at + (slice(None), slice(0, width))] = sent[r : r + 1, :]
    copies = exchange(sent5, srecv, ext_face, ext_face, send_sem, recv_sem, 3 * n_o)
    force_ref[...] = lax.dot_general(
        eg_ref[...], expand_mat(slots, lanes), (NT, ((), ())),
        precision=lax.Precision.HIGHEST, preferred_element_type=F32,
    )
    fold5[...] = sent5[inner]
    for o, copy in zip(OFFSETS, copies):
        copy.wait()
        at = face(opposite(o), dims)
        fold5[at] = fold5[at] + srecv[halo(o, dims)]
    for r, at in enumerate(itertools.product(*[range(d) for d in dims])):
        force_ref[r : r + 1, :] = force_ref[r : r + 1, :] - fold5[at]
    for i in range(X * Y):
        for k in range(3):
            out_ref[i // Y, i % Y, k] = force_ref[pl.ds(i * Z, Z), k * slots : (k + 1) * slots]


def shards(positions, species, neighbors, edge_mask, species_embed, radial_weight, mix_weight, readout, energy_offset):
    X, Y, Z, slots, edges = neighbors.shape
    dims = (X, Y, Z)
    cells = X * Y * Z
    atoms = cells * slots
    lanes = slots * edges
    ns, c = species_embed.shape
    nb = radial_weight.shape[1]
    ext = (X + 2, Y + 2, Z + 2)
    rows = ext[0] * ext[1] * ext[2]
    near = -(-27 * slots // 256) * 256

    vm = pltpu.VMEM
    count = 4 * len(OFFSETS)
    smem = pl.BlockSpec(memory_space=pltpu.SMEM)
    both = pl.pallas_call(
        functools.partial(kernel, dims, slots, edges, nb),
        out_shape=jax.ShapeDtypeStruct((X, Y, 4, Z, slots), F32),
        in_specs=[VM] * 8 + [smem],
        out_specs=VM,
        scratch_shapes=[
            vm(dims + (1, lanes), F32),
            vm((cells, lanes), F32),
            vm((cells, lanes), jnp.int32),
            vm((1, atoms), jnp.int32),
            vm((cells, lanes), F32),
            vm(ext + (1, lanes), F32),
            vm((rows, lanes), F32),
            vm((cells, 3 * lanes), F32),
            vm((cells, near, lanes), BF16),
            vm((cells, rows, lanes), BF16),
            vm((cells, 8, lanes), F32),
            vm((cells, 18 * slots, lanes), BF16),
            vm((ns * nb, 3 * c), F32),
            vm((9, atoms, ns * nb), F32),
            vm((2, 9, atoms, c), F32),
            vm((9, atoms, c), F32),
            vm((atoms, c), F32),
            vm(dims + (slots, c), F32),
            vm(ext + (slots, c), F32),
            vm((cells * lanes, 3 * c), F32),
            vm((cells * lanes, c), F32),
            vm((cells, 3, 2 * lanes, c), BF16),
            vm((cells, 2 * lanes, 3 * c), BF16),
            vm(ext + (slots, c), F32),
            vm(ext + (slots, c), F32),
            vm((cells, nb, lanes), F32),
            vm((cells, 16, lanes), F32),
            vm(dims + (slots, c), F32),
            vm((cells, 3 * lanes), F32),
            vm((rows, 4 * slots), F32),
            vm(ext + (1, lanes), F32),
            vm(ext + (1, lanes), F32),
            vm(dims + (1, lanes), F32),
            pltpu.SemaphoreType.DMA((count,)),
            pltpu.SemaphoreType.DMA((count,)),
            pltpu.SemaphoreType.DMA((2,)),
        ],
        compiler_params=pltpu.CompilerParams(
            collective_id=1, has_side_effects=True, vmem_limit_bytes=58 * 1024 * 1024
        ),
        name="potential",
    )(
        jnp.transpose(positions, (0, 1, 4, 2, 3)), species, neighbors, edge_mask, species_embed,
        radial_weight, mix_weight, readout.reshape(1, c), energy_offset,
    )
    return both[:, :, 3], jnp.transpose(both[:, :, :3], (0, 1, 3, 4, 2))


def solution(mesh):
    g = P("gx", "gy", "gz")
    return jax.shard_map(
        shards,
        mesh=mesh,
        in_specs=(g, g, g, g, P(), P(), P(), P(), P()),
        out_specs=(g, g),
        check_vma=False,
    )
```
